512 devices in a mesh: rep: 16 (over z_lo, x, core), shard: 32 (over y, z_hi).
Axes of the slice: x: 4, y: 8, z: 8 (z_hi: 4, z_lo: 2; z = z_hi * 2 + z_lo), core: 2. Of those that a mesh axis runs over, the one named last changes fastest.
Arguments:
- features: bfloat16 [1, 16, 4096, 8192], P(None, 'rep', 'shard'), may hold values from -6 to 6
- out_grads: bfloat16 [1, 16, 4096, 1024], P(None, 'rep', 'shard'), may hold values from -6 to 6
- doc_ids: int32 [1, 16, 4096], P(None, 'rep', 'shard'), may hold values from 0 to 15, never falling along the last dimension, each value on 1 to 512 neighbouring positions
- offsets: int32 [1, 16, 128], P(None, None, 'shard'), may hold values from 0 to 15
- momentum: bfloat16 [16, 1024, 8192], P('rep', None, 'shard'), may hold values from -6 to 6
Outputs:
- residual_momentum: bfloat16 [16, 1024, 8192], P('rep', None, 'shard')
- update: bfloat16 [1, 1024, 8192], P(None, None, 'shard')
The draws below stay inside these ranges and needn't reach their ends.
Inputs may be any that keep to these rules, and one draw needn't show every extreme that they name: `doc_ids`: along each step's and group's tokens the document number never falls; every number from 0 to 15 occurs, none more than 512 times.
All inputs are finite; a program needn't handle non-finite values.
Results may differ from the reference program's by a relative error of at most 0.012.
Values may be sent and summed in bfloat16 or wider, within the bound.
No kernel may reach another device: no remote copies, remote signals or barrier semaphores. Data moves between devices by JAX's collectives and lax.ppermute only.
A program may use at most 64 MiB of HBM per device.

```python
import math
import jax
import jax.numpy as jnp
import numpy as np
from jax import lax

D = 8192
PANEL = 1024
BLOCK = 64
STRIDE = 16
STEPS = 1
DOCS = 16
TOKENS_G = 4096
GROUPS = 16
DOC_MOST = 512


def with_ends(values, stream_key, smallest, high):
    longest = values.shape.index(max(values.shape))
    spots = []
    for shift in (0, 1):
        where = [jax.random.randint(jax.random.fold_in(stream_key, axis), (), 0, length) for axis, length in enumerate(values.shape)]
        where[longest] = (where[longest] + shift) % values.shape[longest]
        spots.append(tuple(where))
    return values.at[spots[0]].set(smallest).at[spots[1]].set(high)


def levels(own_key, dims, shards, low, top_value):
    def one(dim, shards_of):
        steps = jax.random.uniform(jax.random.fold_in(jax.random.fold_in(own_key, 6), dim), (shards_of,), jnp.float32, low / len(shards), top_value / len(shards))
        return jnp.repeat(jnp.exp(steps), dims[dim] // shards_of).reshape((-1,) + (1,) * (len(dims) - dim - 1))

    gain = one(*shards[0])
    for cut in shards[1:]:
        gain = gain * one(*cut)
    return gain


def profile(amount, total, limit, skew):
    weights = [(1 << 20) // math.isqrt(standing ** skew) + 1 for standing in range(2, amount + 1)]
    rest, holding = total - limit - (amount - 1), [1] * (amount - 1)
    while rest > 0:
        free = [i for i in range(amount - 1) if holding[i] < limit]
        pool, budget = sum([weights[i] for i in free]), rest
        for i in free:
            more = min(limit - holding[i], max(1, budget * weights[i] // pool), rest)
            holding[i] = holding[i] + more
            rest = rest - more
    return np.array([limit] + holding)


def uneven(own_key, amount, total, limit, skew):
    if amount == 2:
        one = jax.random.randint(own_key, (), max(1, total - limit), min(limit, total - 1) + 1)
        return jnp.stack([one, total - one])
    sizes = jnp.asarray(profile(amount, total, limit, skew), jnp.int32)
    pairs = (amount - 1) // 2
    giver, sink = sizes[1:1 + 2 * pairs:2], sizes[2:2 + 2 * pairs:2]
    room = jnp.minimum(giver - 1, limit - sink)
    moved = jax.random.randint(jax.random.fold_in(own_key, 1), (pairs,), 0, 1 << 20) % (room + 1)
    sizes = sizes.at[1:1 + 2 * pairs:2].set(giver - moved).at[2:2 + 2 * pairs:2].set(sink + moved)
    return sizes[jax.random.permutation(jax.random.fold_in(own_key, 2), amount)]


def noise(key, dims, scale, most, split=(), held_as=jnp.bfloat16):
    values = scale * jax.random.normal(key, dims, jnp.float32)
    if split:
        values = values * levels(key, dims, split, -0.22, 0.18)
    return jnp.clip(values, -most, most).astype(held_as)


def setup_inputs(seed: int = 0) -> dict:
    streams_of = jax.random.split(jax.random.key(seed), 6)
    features = noise(streams_of[0], (STEPS, GROUPS, TOKENS_G, D), 1.0, 6.0, ((1, 16), (2, 32)))
    out_grads = noise(streams_of[1], (STEPS, GROUPS, TOKENS_G, PANEL), 1.0, 6.0, ((1, 16), (2, 32)))
    doc_ids = jax.vmap(lambda own: jnp.searchsorted(jnp.cumsum(uneven(own, DOCS, TOKENS_G, DOC_MOST, 0)), jnp.arange(TOKENS_G), side="right"))(jax.random.split(streams_of[2], STEPS * GROUPS)).reshape((STEPS, GROUPS, TOKENS_G)).astype(jnp.int32)
    offsets = with_ends(jax.random.randint(streams_of[3], (STEPS, PANEL // BLOCK, D // BLOCK), 0, STRIDE), jax.random.fold_in(streams_of[3], 1), 0, STRIDE - 1).astype(jnp.int32)
    momentum = noise(streams_of[4], (GROUPS, PANEL, D), 1.0, 6.0, ((0, 16), (2, 32)))
    return {"features": features, "out_grads": out_grads, "doc_ids": doc_ids, "offsets": offsets, "momentum": momentum}


BETA = 0.9
CLIP = 2.0
EPS = 1e-06
PRECISE = lax.Precision.HIGHEST

def dct_table(size):
    freq = lax.broadcasted_iota(jnp.float32, (size, size), 0)
    place = lax.broadcasted_iota(jnp.float32, (size, size), 1)
    matrix = jnp.cos(math.pi * (2.0 * place + 1.0) * freq / (2.0 * size)) * math.sqrt(2.0 / size)
    return jnp.where(freq == 0, matrix / math.sqrt(2.0), matrix)

def forward(moment, matrix):
    blocks = moment.reshape(PANEL // BLOCK, BLOCK, D // BLOCK, BLOCK)
    spectrum = jnp.einsum('ku,aubv,lv->akbl', matrix, blocks, matrix, precision=PRECISE)
    return spectrum.reshape(PANEL, D)

def inverse(spectrum, matrix):
    blocks = spectrum.reshape(PANEL // BLOCK, BLOCK, D // BLOCK, BLOCK)
    spatial = jnp.einsum('ku,akbl,lv->aubv', matrix, blocks, matrix, precision=PRECISE)
    return spatial.reshape(PANEL, D)

def selector_for(offsets_step):
    grouped = jnp.repeat(offsets_step, BLOCK // STRIDE, axis=1)
    row_index = jnp.arange(BLOCK, dtype=jnp.int32)
    shift_amount = (grouped[:, None, :] - row_index[None, :, None]) % STRIDE
    residue = jnp.arange(STRIDE, dtype=jnp.int32)
    return (residue == shift_amount[..., None]).astype(jnp.float32)

def pack_entries(spectrum, selector):
    shaped = spectrum.reshape(PANEL // BLOCK, BLOCK, D // STRIDE, STRIDE)
    return lax.optimization_barrier(jnp.sum(shaped * selector, axis=-1))

def place_entries(packed, selector):
    return (packed[..., None] * selector).reshape(PANEL, D)

def expand_scale(block_scale):
    return jnp.repeat(block_scale.astype(jnp.float32), BLOCK // STRIDE, axis=-1)[..., None, :]

def compress(packed):
    shaped = packed.reshape(PANEL // BLOCK, BLOCK, D // BLOCK, BLOCK // STRIDE)
    mean_square = lax.optimization_barrier(jnp.mean(shaped * shaped, axis=(1, 3)))
    block_scale = (CLIP * jnp.sqrt(mean_square + EPS)).astype(jnp.bfloat16)
    spread = expand_scale(block_scale)
    quantized = jnp.clip(packed / spread, -1.0, 1.0).astype(jnp.bfloat16)
    return quantized.astype(jnp.float32) * spread

def reference(features, out_grads, doc_ids, offsets, momentum):
    matrix = dct_table(BLOCK)
    selectors = [selector_for(offsets[index]) for index in range(STEPS)]

    def one_group(inputs):
        group_rows, group_grads, group_ids, start_moment = inputs
        moment = start_moment.astype(jnp.float32)
        decoded_steps = []
        for index in range(STEPS):
            onehot = (group_ids[index][:, None] == jnp.arange(DOCS, dtype=jnp.int32)[None, :]).astype(jnp.float32)
            lengths = lax.optimization_barrier(jnp.sum(onehot, axis=0))
            token_weight = lax.optimization_barrier(jnp.sum(onehot / lengths[None, :], axis=1))
            scaled = (group_grads[index].astype(jnp.float32) * token_weight[:, None]).astype(jnp.bfloat16)
            gradient = lax.dot_general(scaled, group_rows[index], (((0,), (0,)), ((), ())), preferred_element_type=jnp.float32).astype(jnp.bfloat16)
            moment = BETA * moment + gradient.astype(jnp.float32)
            spectrum = forward(moment, matrix)
            packed = pack_entries(spectrum, selectors[index])
            decoded = compress(packed)
            moment = moment - inverse(place_entries(decoded, selectors[index]), matrix)
            decoded_steps.append(decoded)
        return (moment.astype(jnp.bfloat16), jnp.stack(decoded_steps))
    residual_momentum, decoded_all = lax.map(one_group, (jnp.moveaxis(features, 1, 0), jnp.moveaxis(out_grads, 1, 0), jnp.moveaxis(doc_ids, 1, 0), momentum))
    average = lax.optimization_barrier(jnp.sum(decoded_all, axis=0)) / GROUPS
    update = jnp.stack([inverse(place_entries(average[index], selectors[index]), matrix).astype(jnp.bfloat16) for index in range(STEPS)])
    return (residual_momentum, update)
```

```python
import math

import jax
import jax.numpy as jnp
import numpy as np
from jax import lax
from jax.experimental import pallas as pl
from jax.experimental.pallas import tpu as pltpu
from jax.sharding import PartitionSpec as P

BLOCK = 64
STRIDE = 16
DOCS = 16
LINES = 8
BETA = 0.9
CLIP = 2.0
EPS = 1e-06


TILE = 256


def dct_parts():
    freq = np.arange(BLOCK, dtype=np.float64)[:, None]
    place = np.arange(BLOCK, dtype=np.float64)[None, :]
    table = np.cos(math.pi * (2.0 * place + 1.0) * freq / (2.0 * BLOCK)) * math.sqrt(2.0 / BLOCK)
    table[0] /= math.sqrt(2.0)
    whole = np.kron(np.eye(TILE // BLOCK), table)
    high = whole.astype(jnp.bfloat16)
    low = (whole - high.astype(np.float64)).astype(jnp.bfloat16)
    return jnp.asarray(high), jnp.asarray(low)


def dot(a, b, dims):
    return lax.dot_general(a, b, (dims, ((), ())), preferred_element_type=jnp.float32)


def split(x):
    high = x.astype(jnp.bfloat16)
    return high, (x - high.astype(jnp.float32)).astype(jnp.bfloat16)


def left(table, x, dim):
    (th, tl), (xh, xl) = table, split(x)
    dims = ((dim,), (0,))
    return dot(th, xh, dims) + (dot(th, xl, dims) + dot(tl, xh, dims))


def right(x, table, dim):
    (th, tl), (xh, xl) = table, split(x)
    dims = ((1,), (dim,))
    return dot(xh, th, dims) + (dot(xl, th, dims) + dot(xh, tl, dims))


def selected(offsets):
    count, width = offsets.shape
    shape = (count, BLOCK, width)
    both = lax.broadcasted_iota(jnp.int32, shape, 1) + lax.broadcasted_iota(jnp.int32, shape, 2)
    return ((both % STRIDE) == offsets[:, None, :]).reshape(count * BLOCK, width)


def forward_kernel(moment, offsets, high, low, ones, decoded, sent, packed):
    table = (high[...], low[...])
    per = TILE // BLOCK
    rows = TILE // STRIDE
    for i in range(moment.shape[0] // TILE):
        spectrum = right(left(table, moment[i * TILE : (i + 1) * TILE], 1), table, 1)
        kept = jnp.where(selected(offsets[i * per : (i + 1) * per]), spectrum, 0.0)
        packed[i * rows : (i + 1) * rows] = jnp.sum(kept.reshape(rows, STRIDE, TILE), axis=1)
    values = packed[...]
    group = BLOCK // STRIDE
    squares = jnp.sum((values * values).reshape(-1, group, TILE), axis=1)
    first = squares.astype(jnp.bfloat16)
    rest = squares - first.astype(jnp.float32)
    second, third = split(rest)
    dims = ((1,), (0,))
    total = dot(first, ones[...], dims) + (dot(second, ones[...], dims) + dot(third, ones[...], dims))
    mean = total * (1.0 / (BLOCK * group))
    scale = (CLIP * jnp.sqrt(mean + EPS)).astype(jnp.bfloat16).astype(jnp.float32)
    spread = jnp.broadcast_to(scale[:, None, :], (scale.shape[0], group, TILE)).reshape(values.shape)
    quantized = jnp.clip(values / spread, -1.0, 1.0).astype(jnp.bfloat16)
    result = quantized.astype(jnp.float32) * spread
    decoded[...] = result
    sent[...] = result.astype(jnp.bfloat16)


def spread_tile(values, offsets):
    rows, width = values.shape
    wide = jnp.broadcast_to(values[:, None, :], (rows, STRIDE, width)).reshape(rows * STRIDE, width)
    return jnp.where(selected(offsets), wide, 0.0)


def inverse_tile(values, offsets, table):
    return right(left(table, spread_tile(values, offsets), 0), table, 0)


def residual_kernel(moment, decoded, offsets, high, low, out):
    table = (high[...], low[...])
    per = TILE // BLOCK
    rows = TILE // STRIDE
    for i in range(moment.shape[0] // TILE):
        here = slice(i * TILE, (i + 1) * TILE)
        back = inverse_tile(decoded[i * rows : (i + 1) * rows], offsets[i * per : (i + 1) * per], table)
        out[here] = (moment[here] - back).astype(jnp.bfloat16)


def update_kernel(parts, offsets, high, low, out):
    table = (high[...], low[...])
    per = TILE // BLOCK
    rows = TILE // STRIDE
    count = parts.shape[0]
    for i in range(out.shape[0] // TILE):
        here = slice(i * rows, (i + 1) * rows)
        total = parts[0, here].astype(jnp.float32)
        for k in range(1, count):
            total += parts[k, here].astype(jnp.float32)
        back = inverse_tile(total * (1.0 / count), offsets[i * per : (i + 1) * per], table)
        out[i * TILE : (i + 1) * TILE] = back.astype(jnp.bfloat16)


def call(kernel, out_shape, flops, scratch=()):
    return pl.pallas_call(
        kernel,
        out_shape=out_shape,
        scratch_shapes=scratch,
        cost_estimate=pl.CostEstimate(flops=flops, bytes_accessed=2 << 20, transcendentals=0),
    )


def body(features, out_grads, doc_ids, offsets, momentum):
    shards = lax.axis_size("shard")
    deep = shards // LINES
    groups = lax.axis_size("rep")
    line = lax.axis_index("shard") // deep

    def along_line(x, k):
        pairs = [(y * deep + z, y * deep + (z + k) % deep) for y in range(LINES) for z in range(deep)]
        return lax.ppermute(x, "shard", pairs)

    def across(x, k):
        pairs = [(y * deep + z, (y + k) % LINES * deep + z) for y in range(LINES) for z in range(deep)]
        return lax.ppermute(x, "shard", pairs)

    order = [deep // 2] + [k for k in range(1, deep) if k != deep // 2]
    rows = features[0, 0]
    grads = out_grads[0, 0]
    tokens, panel = grads.shape
    width = rows.shape[1] // shards

    with jax.named_scope("grads"):
        all_grads = [grads] + [along_line(grads, k) for k in order]

    onehot = (doc_ids[0, 0][:, None] == jnp.arange(128, dtype=jnp.int32)[None, :]).astype(jnp.float32)
    counts = jnp.broadcast_to(jnp.sum(onehot, axis=0, keepdims=True), (8, 128))
    with jax.named_scope("counts"):
        before, after = across(counts, 1), across(counts, -1)
    lanes = jnp.concatenate([counts[:1, :16], before[:1, :16], after[:1, :16]], axis=1)
    extra = jnp.concatenate(
        [onehot[:, :16], jnp.broadcast_to(lanes, (tokens, 48)), jnp.zeros((tokens, 64), jnp.float32)], axis=1
    ).astype(jnp.bfloat16)

    blocks = jnp.moveaxis(rows.reshape(tokens, LINES, deep, width), 0, 2)
    blocks = lax.optimization_barrier(blocks)
    me_deep = lax.axis_index("shard") % deep

    def piece(owner, k):
        at = (line + owner) % LINES
        z = (me_deep + k) % deep
        return lax.dynamic_slice(blocks, (at, z, 0, 0), (1, 1, tokens, width)).reshape(tokens, width)

    def chunk(owners, tail=None):
        got = []
        for k in [0] + order:
            parts = [piece(owner, k) for owner in owners]
            if tail is not None:
                parts.append(tail)
            sent = jnp.concatenate(parts, axis=1) if len(parts) > 1 else parts[0]
            got.append(sent if k == 0 else along_line(sent, k))
        return jnp.concatenate(got, axis=0)

    with jax.named_scope("chunk4"):
        far = chunk([4], extra)
    with jax.named_scope("chunk3"):
        third = chunk([3, -3])
    with jax.named_scope("chunk2"):
        second = chunk([2, -2])
    with jax.named_scope("chunk1"):
        first = chunk([1, -1, 0])

    notes = far[:, width:].astype(jnp.float32)
    heads = sum(notes[i * tokens, 16:64] for i in range(deep))
    lengths = heads[:16] + heads[16:32] + heads[32:]
    token_weight = jnp.sum(notes[:, :16] / jnp.maximum(lengths, 1.0)[None, :], axis=1)
    scaled = (jnp.concatenate(all_grads, axis=0).astype(jnp.float32) * token_weight[:, None]).astype(jnp.bfloat16)

    def product(columns, part=slice(None)):
        return dot(scaled[:, part], columns, ((0,), (0,)))

    half = panel // 2
    with jax.named_scope("ring4"):
        up = across(product(far[:, :width], slice(0, half)).astype(jnp.bfloat16), 1)
        down = across(product(far[:, :width], slice(half, panel)).astype(jnp.bfloat16), -1)
    with jax.named_scope("ring3"):
        none = jnp.zeros((half, width), jnp.float32)
        up = product(third[:, :width]) + jnp.concatenate([up.astype(jnp.float32), none], axis=0)
        down = product(third[:, width:]) + jnp.concatenate([none, down.astype(jnp.float32)], axis=0)
        up, down = across(up.astype(jnp.bfloat16), 1), across(down.astype(jnp.bfloat16), -1)
    with jax.named_scope("ring2"):
        up = product(second[:, :width]) + up.astype(jnp.float32)
        down = product(second[:, width:]) + down.astype(jnp.float32)
        up, down = across(up.astype(jnp.bfloat16), 1), across(down.astype(jnp.bfloat16), -1)
    with jax.named_scope("ring1"):
        up = product(first[:, :width]) + up.astype(jnp.float32)
        down = product(first[:, width : 2 * width]) + down.astype(jnp.float32)
        up, down = across(up.astype(jnp.bfloat16), 1), across(down.astype(jnp.bfloat16), -1)
    summed = product(first[:, 2 * width :]) + up.astype(jnp.float32) + down.astype(jnp.float32)
    gradient = summed.astype(jnp.bfloat16)
    moment = BETA * momentum[0].astype(jnp.float32) + gradient.astype(jnp.float32)

    high, low = dct_parts()
    ones = jnp.asarray(np.kron(np.eye(TILE // BLOCK), np.ones((BLOCK, BLOCK))), jnp.bfloat16)
    wide = jnp.repeat(offsets[0], BLOCK, axis=1)
    kept = panel // STRIDE
    flops = 6 * 2 * 2 * panel * TILE * TILE
    decoded, sent = call(
        forward_kernel,
        (jax.ShapeDtypeStruct((kept, width), jnp.float32), jax.ShapeDtypeStruct((kept, width), jnp.bfloat16)),
        flops,
        (pltpu.VMEM((kept, width), jnp.float32),),
    )(moment, wide, high, low, ones)
    with jax.named_scope("share"):
        parts = lax.all_to_all(jnp.broadcast_to(sent[None], (groups, kept, width)), "rep", 0, 0, tiled=True)
    residual = call(residual_kernel, jax.ShapeDtypeStruct((panel, width), jnp.bfloat16), flops)(
        moment, decoded, wide, high, low
    )
    update = call(update_kernel, jax.ShapeDtypeStruct((panel, width), jnp.bfloat16), flops)(
        parts, wide, high, low
    )
    return residual[None], update[None]


def solution(mesh):
    return jax.shard_map(
        body,
        mesh=mesh,
        in_specs=(
            P(None, "rep", "shard", None),
            P(None, "rep", "shard", None),
            P(None, "rep", "shard"),
            P(None, None, "shard"),
            P("rep", None, "shard"),
        ),
        out_specs=(P("rep", None, "shard"), P(None, None, "shard")),
        check_vma=False,
    )
```

```python
import functools
import math

import jax
import jax.numpy as jnp
import numpy as np
from jax import lax
from jax.experimental import pallas as pl
from jax.experimental.pallas import tpu as pltpu
from jax.sharding import PartitionSpec as P


BLOCK = 64
STRIDE = 16
DOCS = 16
LINES = 8
BETA = 0.9
CLIP = 2.0
EPS = 1e-06


TILE = 256
GRANT = 16 << 20
FULL = 60 << 20


def dct_parts():
    freq = np.arange(BLOCK, dtype=np.float64)[:, None]
    place = np.arange(BLOCK, dtype=np.float64)[None, :]
    table = np.cos(math.pi * (2.0 * place + 1.0) * freq / (2.0 * BLOCK)) * math.sqrt(2.0 / BLOCK)
    table[0] /= math.sqrt(2.0)
    whole = np.kron(np.eye(TILE // BLOCK), table)
    high = whole.astype(jnp.bfloat16)
    low = (whole - high.astype(np.float64)).astype(jnp.bfloat16)
    return jnp.asarray(high), jnp.asarray(low)


def dot(a, b, dims):
    return lax.dot_general(a, b, (dims, ((), ())), preferred_element_type=jnp.float32)


def split(x):
    high = x.astype(jnp.bfloat16)
    return high, (x - high.astype(jnp.float32)).astype(jnp.bfloat16)


def left(table, x, dim):
    (th, tl), (xh, xl) = table, split(x)
    dims = ((dim,), (0,))
    return dot(th, xh, dims) + (dot(th, xl, dims) + dot(tl, xh, dims))


def right(x, table, dim):
    (th, tl), (xh, xl) = table, split(x)
    dims = ((1,), (dim,))
    return dot(xh, th, dims) + (dot(xl, th, dims) + dot(xh, tl, dims))


def selected(offsets):
    count, width = offsets.shape
    shape = (count, BLOCK, width)
    both = lax.broadcasted_iota(jnp.int32, shape, 1) + lax.broadcasted_iota(jnp.int32, shape, 2)
    return ((both & (STRIDE - 1)) == offsets[:, None, :]).reshape(count * BLOCK, width)


def gathered(exchanged, start, size):
    deep = exchanged.shape[0]
    z = lax.axis_index("shard") % deep
    return jnp.concatenate([exchanged[(z - k + deep) % deep, :, start : start + size] for k in range(deep)], axis=0)


def joined(parts, start, size):
    return jnp.concatenate([part[:, start : start + size] for part in parts], axis=0)


def fetch(rows, deep, width, moves, sem):
    me = lax.axis_index("shard")
    line = me // deep
    copies = []
    for i, (owner, z, target) in enumerate(moves):
        block = (line + owner + LINES) % LINES * deep + z
        column = pl.multiple_of(block * width, width)
        copies.append(pltpu.make_async_copy(rows.at[:, pl.ds(column, width)], target, sem.at[i]))
    for copy in copies:
        copy.start()
    return copies


def early_kernel(rows, grads, out, sem):
    deep = out.shape[0]
    panel = grads.shape[1]
    width = out.shape[2] - panel
    moves = [(4, z, out.at[z, :, pl.ds(panel, width)]) for z in range(deep)]
    copies = fetch(rows, deep, width, moves, sem)
    for z in range(deep):
        out[z, :, :panel] = grads[...]
    for copy in copies:
        copy.wait()


def late_kernel(rows, extra, *rest):
    deep = 4
    third, second, last, sem = rest[:deep], rest[deep : 2 * deep], rest[2 * deep], rest[2 * deep + 1]
    width = last.shape[2] // 3
    me = lax.axis_index("shard") % deep
    moves = []
    for k in range(deep):
        z = (me + k) % deep
        for j, owner in enumerate((3, -3)):
            moves.append((owner, z, third[k].at[:, pl.ds(j * width, width)]))
    for k in range(deep):
        z = (me + k) % deep
        for j, owner in enumerate((2, -2)):
            moves.append((owner, z, second[k].at[:, pl.ds(j * width, width)]))
    for z in range(deep):
        for j, owner in enumerate((1, -1, 0)):
            moves.append((owner, z, last.at[z, :, pl.ds(j * width, width)]))
    copies = fetch(rows, deep, width, moves, sem)
    for k in range(deep):
        third[k][:, 2 * width :] = extra[...]
    for copy in copies:
        copy.wait()


def scale_kernel(exchanged, *rest):
    notes, out = rest[:-1], rest[-1]
    deep, tokens = exchanged.shape[0], exchanged.shape[1]
    width = notes[0].shape[1] - 128
    panel = exchanged.shape[2] - width // 2
    z = lax.axis_index("shard") % deep
    marks = [note[:, width:].astype(jnp.float32) for note in notes]
    heads = marks[0][:8]
    for mark in marks[1:]:
        heads = heads + mark[:8]
    lengths = pltpu.roll(heads, 112, 1) + pltpu.roll(heads, 96, 1) + pltpu.roll(heads, 80, 1)
    share = 1.0 / jnp.maximum(lengths[:1], 1.0)
    lane = lax.broadcasted_iota(jnp.int32, (tokens, 128), 1)
    for k in range(deep):
        weight = jnp.sum(jnp.where(lane < DOCS, marks[k] * share, 0.0), axis=1, keepdims=True)
        block = exchanged[(z - k + deep) % deep, :, :panel].astype(jnp.float32)
        out[:, k * tokens : (k + 1) * tokens] = (block * weight).T.astype(jnp.bfloat16)


def far_kernel(weights, exchanged, up, down):
    half = up.shape[0]
    columns = gathered(exchanged, exchanged.shape[2] - up.shape[1], up.shape[1])
    dims = ((1,), (0,))
    up[...] = dot(weights[:half], columns, dims).astype(jnp.bfloat16)
    down[...] = dot(weights[half:], columns, dims).astype(jnp.bfloat16)


def near_kernel(start, top, pieces, weights, received, *rest):
    parts, out = rest[:-1], rest[-1]
    width = out.shape[1]
    columns = joined(parts, start, width) if pieces else gathered(parts[0], start, width)
    total = dot(weights[...], columns, ((1,), (0,)))
    rows = received.shape[0]
    if rows == out.shape[0]:
        out[...] = (total + received[...].astype(jnp.float32)).astype(jnp.bfloat16)
    else:
        here, other = (slice(0, rows), slice(rows, None)) if top else (slice(rows, None), slice(0, rows))
        out[here] = (total[here] + received[...].astype(jnp.float32)).astype(jnp.bfloat16)
        out[other] = total[other].astype(jnp.bfloat16)


def forward_kernel(weights, exchanged, up, down, momentum, offsets, high, low, ones, summed, decoded, sent, packed):
    table = (high[...], low[...])
    per = TILE // BLOCK
    rows = TILE // STRIDE
    width = summed.shape[1]
    columns = gathered(exchanged, 2 * width, width)
    for i in range(summed.shape[0] // TILE):
        here = slice(i * TILE, (i + 1) * TILE)
        total = dot(weights[here], columns, ((1,), (0,)))
        total = total + up[here].astype(jnp.float32) + down[here].astype(jnp.float32)
        gradient = total.astype(jnp.bfloat16)
        summed[here] = gradient
        value = BETA * momentum[here].astype(jnp.float32) + gradient.astype(jnp.float32)
        spectrum = right(left(table, value, 1), table, 1)
        kept = jnp.where(selected(offsets[i * per : (i + 1) * per]), spectrum, 0.0)
        packed[i * rows : (i + 1) * rows] = jnp.sum(kept.reshape(rows, STRIDE, TILE), axis=1)
    values = packed[...]
    group = BLOCK // STRIDE
    squares = jnp.sum((values * values).reshape(-1, group, TILE), axis=1)
    first = squares.astype(jnp.bfloat16)
    rest = squares - first.astype(jnp.float32)
    second, third = split(rest)
    dims = ((1,), (0,))
    total = dot(first, ones[...], dims) + (dot(second, ones[...], dims) + dot(third, ones[...], dims))
    mean = total * (1.0 / (BLOCK * group))
    scale = (CLIP * jnp.sqrt(mean + EPS)).astype(jnp.bfloat16).astype(jnp.float32)
    spread = jnp.broadcast_to(scale[:, None, :], (scale.shape[0], group, TILE)).reshape(values.shape)
    quantized = jnp.clip(values / spread, -1.0, 1.0).astype(jnp.bfloat16)
    result = quantized.astype(jnp.float32) * spread
    decoded[...] = result
    rounded = result.astype(jnp.bfloat16)
    for k in range(sent.shape[0]):
        sent[k] = rounded


def spread_tile(values, offsets):
    rows, width = values.shape
    wide = jnp.broadcast_to(values[:, None, :], (rows, STRIDE, width)).reshape(rows * STRIDE, width)
    return jnp.where(selected(offsets), wide, 0.0)


def inverse_tile(values, offsets, table):
    return right(left(table, spread_tile(values, offsets), 0), table, 0)


def residual_kernel(momentum, summed, decoded, offsets, high, low, out):
    table = (high[...], low[...])
    per = TILE // BLOCK
    rows = TILE // STRIDE
    for i in range(out.shape[0] // TILE):
        here = slice(i * TILE, (i + 1) * TILE)
        value = BETA * momentum[here].astype(jnp.float32) + summed[here].astype(jnp.float32)
        back = inverse_tile(decoded[i * rows : (i + 1) * rows], offsets[i * per : (i + 1) * per], table)
        out[here] = (value - back).astype(jnp.bfloat16)


def update_kernel(parts, offsets, high, low, out):
    table = (high[...], low[...])
    per = TILE // BLOCK
    rows = TILE // STRIDE
    count = parts.shape[0]
    for i in range(out.shape[0] // TILE):
        here = slice(i * rows, (i + 1) * rows)
        total = parts[0, here].astype(jnp.float32)
        for k in range(1, count):
            total += parts[k, here].astype(jnp.float32)
        back = inverse_tile(total * (1.0 / count), offsets[i * per : (i + 1) * per], table)
        out[i * TILE : (i + 1) * TILE] = back.astype(jnp.bfloat16)


def call(kernel, out_shape, flops, scratch=(), in_specs=None, grant=GRANT):
    extra = {} if in_specs is None else {"in_specs": in_specs}
    return pl.pallas_call(
        kernel,
        out_shape=out_shape,
        scratch_shapes=scratch,
        compiler_params=pltpu.CompilerParams(vmem_limit_bytes=grant),
        cost_estimate=pl.CostEstimate(flops=flops, bytes_accessed=2 << 20, transcendentals=0),
        **extra,
    )


def shaped(*shape, dtype=jnp.bfloat16):
    return jax.ShapeDtypeStruct(shape, dtype)


def step(features, out_grads, doc_ids, offsets, momentum):
    shards = lax.axis_size("shard")
    deep = shards // LINES
    groups = lax.axis_size("rep")

    def along_line(x, k):
        pairs = [(y * deep + z, y * deep + (z + k) % deep) for y in range(LINES) for z in range(deep)]
        return lax.ppermute(x, "shard", pairs)

    def across(x, k):
        pairs = [(y * deep + z, (y + k) % LINES * deep + z) for y in range(LINES) for z in range(deep)]
        return lax.ppermute(x, "shard", pairs)

    def exchange(x):
        lines = [[y * deep + z for z in range(deep)] for y in range(LINES)]
        return lax.all_to_all(x, "shard", 0, 0, axis_index_groups=lines, tiled=True)

    rows = features[0, 0]
    grads = out_grads[0, 0]
    tokens, panel = grads.shape
    width = rows.shape[1] // shards
    whole = pl.BlockSpec(memory_space=pltpu.VMEM)
    apart = pl.BlockSpec(memory_space=pltpu.HBM)
    work = 2 * panel * deep * tokens * width

    early = call(
        early_kernel,
        shaped(deep, tokens, panel + width),
        work,
        (pltpu.SemaphoreType.DMA((deep,)),),
        [apart, whole],
        FULL,
    )(rows, grads)
    early = exchange(early)

    onehot = (doc_ids[0, 0][:, None] == jnp.arange(128, dtype=jnp.int32)[None, :]).astype(jnp.float32)
    counts = jnp.broadcast_to(jnp.sum(onehot, axis=0, keepdims=True), (8, 128))
    before = across(counts, 1)
    after = across(counts, -1)
    lanes = jnp.concatenate([counts[:1, :16], before[:1, :16], after[:1, :16]], axis=1)
    extra = jnp.concatenate(
        [onehot[:, :16], jnp.broadcast_to(lanes, (tokens, 48)), jnp.zeros((tokens, 64), jnp.float32)], axis=1
    ).astype(jnp.bfloat16)

    outs = call(
        late_kernel,
        [shaped(tokens, 2 * width + 128)] * deep + [shaped(tokens, 2 * width)] * deep + [shaped(deep, tokens, 3 * width)],
        work,
        (pltpu.SemaphoreType.DMA((7 * deep,)),),
        [apart, whole],
        FULL,
    )(rows, extra)
    third, second, last = list(outs[:deep]), list(outs[deep : 2 * deep]), outs[2 * deep]
    for k in (2, 1, 3):
        third[k] = along_line(third[k], k)
    for k in (2, 1, 3):
        second[k] = along_line(second[k], k)
    last = exchange(last)

    weights = call(scale_kernel, shaped(panel, deep * tokens), work)(early, *third)
    half = panel // 2
    up, down = call(far_kernel, [shaped(half, width)] * 2, work)(weights, early)

    def ring(up, down):
        up = across(up, 1)
        down = across(down, -1)
        return up, down

    def near(start, top, received, parts):
        kernel = functools.partial(near_kernel, start, top, len(parts) > 1)
        return call(kernel, shaped(panel, width), work)(weights, received, *parts)

    up, down = ring(up, down)
    up, down = ring(near(0, True, up, third), near(width, False, down, third))
    up, down = ring(near(0, True, up, second), near(width, False, down, second))
    up, down = ring(near(0, True, up, [last]), near(width, False, down, [last]))

    high, low = dct_parts()
    ones = jnp.asarray(np.kron(np.eye(TILE // BLOCK), np.ones((BLOCK, BLOCK))), jnp.bfloat16)
    wide = jnp.repeat(offsets[0], BLOCK, axis=1)
    kept = panel // STRIDE
    flops = 6 * 2 * 2 * panel * TILE * TILE
    summed, decoded, sent = call(
        forward_kernel,
        (
            shaped(panel, width),
            shaped(kept, width, dtype=jnp.float32),
            shaped(groups, kept, width),
        ),
        flops,
        (pltpu.VMEM((kept, width), jnp.float32),),
    )(weights, last, up, down, momentum[0], wide, high, low, ones)
    parts = lax.all_to_all(sent, "rep", 0, 0, tiled=True)
    residual = call(residual_kernel, shaped(panel, width), flops)(momentum[0], summed, decoded, wide, high, low)
    update = call(update_kernel, shaped(panel, width), flops)(parts, wide, high, low)
    return residual[None], update[None]


def solution(mesh):
    return jax.shard_map(
        step,
        mesh=mesh,
        in_specs=(
            P(None, "rep", "shard", None),
            P(None, "rep", "shard", None),
            P(None, "rep", "shard"),
            P(None, None, "shard"),
            P("rep", None, "shard"),
        ),
        out_specs=(P("rep", None, "shard"), P(None, None, "shard")),
        check_vma=False,
    )
```

```python
import functools
import math

import jax
import jax.numpy as jnp
import numpy as np
from jax import lax
from jax.experimental import pallas as pl
from jax.experimental.pallas import tpu as pltpu
from jax.sharding import PartitionSpec as P


BLOCK = 64
STRIDE = 16
DOCS = 16
LINES = 8
BETA = 0.9
CLIP = 2.0
EPS = 1e-06


TILE = 256
GRANT = 16 << 20
FULL = 60 << 20


def dct_parts():
    freq = np.arange(BLOCK, dtype=np.float64)[:, None]
    place = np.arange(BLOCK, dtype=np.float64)[None, :]
    table = np.cos(math.pi * (2.0 * place + 1.0) * freq / (2.0 * BLOCK)) * math.sqrt(2.0 / BLOCK)
    table[0] /= math.sqrt(2.0)
    whole = np.kron(np.eye(TILE // BLOCK), table)
    high = whole.astype(jnp.bfloat16)
    low = (whole - high.astype(np.float64)).astype(jnp.bfloat16)
    return jnp.asarray(high), jnp.asarray(low)


def dot(a, b, dims):
    return lax.dot_general(a, b, (dims, ((), ())), preferred_element_type=jnp.float32)


def split(x):
    high = x.astype(jnp.bfloat16)
    return high, (x - high.astype(jnp.float32)).astype(jnp.bfloat16)


def left(table, x, dim):
    (th, tl), (xh, xl) = table, split(x)
    dims = ((dim,), (0,))
    return dot(th, xh, dims) + (dot(th, xl, dims) + dot(tl, xh, dims))


def right(x, table, dim):
    (th, tl), (xh, xl) = table, split(x)
    dims = ((1,), (dim,))
    return dot(xh, th, dims) + (dot(xl, th, dims) + dot(xh, tl, dims))


def selected(offsets):
    count, width = offsets.shape
    shape = (count, BLOCK, width)
    both = lax.broadcasted_iota(jnp.int32, shape, 1) + lax.broadcasted_iota(jnp.int32, shape, 2)
    return ((both & (STRIDE - 1)) == offsets[:, None, :]).reshape(count * BLOCK, width)


def gathered(exchanged, start, size):
    deep = exchanged.shape[0]
    z = lax.axis_index("shard") % deep
    return jnp.concatenate([exchanged[(z - k + deep) % deep, :, start : start + size] for k in range(deep)], axis=0)


def joined(parts, start, size):
    return jnp.concatenate([part[:, start : start + size] for part in parts], axis=0)


def fetch(rows, deep, width, moves, sem):
    me = lax.axis_index("shard")
    line = me // deep
    copies = []
    for i, (owner, z, target) in enumerate(moves):
        block = (line + owner + LINES) % LINES * deep + z
        column = pl.multiple_of(block * width, width)
        copies.append(pltpu.make_async_copy(rows.at[:, pl.ds(column, width)], target, sem.at[i]))
    for copy in copies:
        copy.start()
    return copies


def early_kernel(rows, grads, out, sem):
    deep = out.shape[0]
    panel = grads.shape[1]
    width = out.shape[2] - panel
    moves = [(4, z, out.at[z, :, pl.ds(panel, width)]) for z in range(deep)]
    copies = fetch(rows, deep, width, moves, sem)
    for z in range(deep):
        out[z, :, :panel] = grads[...]
    for copy in copies:
        copy.wait()


def late_kernel(rows, *rest):
    third, (second, last, sem) = rest[:-3], rest[-3:]
    deep = len(third)
    width = last.shape[2] // 3
    me = lax.axis_index("shard") % deep
    moves = []
    for k in range(deep):
        z = (me + k) % deep
        for j, owner in enumerate((3, -3)):
            moves.append((owner, z, third[k].at[:, pl.ds(j * width, width)]))
    for target, owners in ((second, (2, -2)), (last, (1, -1, 0))):
        for z in range(deep):
            for j, owner in enumerate(owners):
                moves.append((owner, z, target.at[z, :, pl.ds(j * width, width)]))
    for copy in fetch(rows, deep, width, moves, sem):
        copy.wait()


def scale_kernel(exchanged, *rest):
    notes, out = rest[:-1], rest[-1]
    deep, tokens = exchanged.shape[0], exchanged.shape[1]
    panel = out.shape[0]
    z = lax.axis_index("shard") % deep
    marks = [note[...].astype(jnp.float32) for note in notes]
    heads = marks[0][:8]
    for mark in marks[1:]:
        heads = heads + mark[:8]
    lengths = pltpu.roll(heads, 112, 1) + pltpu.roll(heads, 96, 1) + pltpu.roll(heads, 80, 1)
    share = 1.0 / jnp.maximum(lengths[:1], 1.0)
    lane = lax.broadcasted_iota(jnp.int32, (tokens, 128), 1)
    for k in range(deep):
        weight = jnp.sum(jnp.where(lane < DOCS, marks[k] * share, 0.0), axis=1, keepdims=True)
        block = exchanged[(z - k + deep) % deep, :, :panel].astype(jnp.float32)
        out[:, k * tokens : (k + 1) * tokens] = (block * weight).T.astype(jnp.bfloat16)


def far_kernel(weights, exchanged, up, down):
    half = up.shape[0]
    columns = gathered(exchanged, exchanged.shape[2] - up.shape[1], up.shape[1])
    dims = ((1,), (0,))
    up[...] = dot(weights[:half], columns, dims).astype(jnp.bfloat16)
    down[...] = dot(weights[half:], columns, dims).astype(jnp.bfloat16)


def near_kernel(start, top, pieces, weights, received, *rest):
    parts, out = rest[:-1], rest[-1]
    width = out.shape[1]
    columns = joined(parts, start, width) if pieces else gathered(parts[0], start, width)
    total = dot(weights[...], columns, ((1,), (0,)))
    rows = received.shape[0]
    if rows == out.shape[0]:
        out[...] = (total + received[...].astype(jnp.float32)).astype(jnp.bfloat16)
    else:
        here, other = (slice(0, rows), slice(rows, None)) if top else (slice(rows, None), slice(0, rows))
        out[here] = (total[here] + received[...].astype(jnp.float32)).astype(jnp.bfloat16)
        out[other] = total[other].astype(jnp.bfloat16)


def forward_kernel(weights, exchanged, up, down, momentum, offsets, high, low, ones, summed, decoded, sent, packed):
    table = (high[...], low[...])
    per = TILE // BLOCK
    rows = TILE // STRIDE
    width = summed.shape[1]
    columns = gathered(exchanged, 2 * width, width)
    for i in range(summed.shape[0] // TILE):
        here = slice(i * TILE, (i + 1) * TILE)
        total = dot(weights[here], columns, ((1,), (0,)))
        total = total + up[here].astype(jnp.float32) + down[here].astype(jnp.float32)
        gradient = total.astype(jnp.bfloat16)
        summed[here] = gradient
        value = BETA * momentum[here].astype(jnp.float32) + gradient.astype(jnp.float32)
        spectrum = right(left(table, value, 1), table, 1)
        kept = jnp.where(selected(offsets[i * per : (i + 1) * per]), spectrum, 0.0)
        packed[i * rows : (i + 1) * rows] = jnp.sum(kept.reshape(rows, STRIDE, TILE), axis=1)
    values = packed[...]
    group = BLOCK // STRIDE
    squares = jnp.sum((values * values).reshape(-1, group, TILE), axis=1)
    first = squares.astype(jnp.bfloat16)
    rest = squares - first.astype(jnp.float32)
    second, third = split(rest)
    dims = ((1,), (0,))
    total = dot(first, ones[...], dims) + (dot(second, ones[...], dims) + dot(third, ones[...], dims))
    mean = total * (1.0 / (BLOCK * group))
    scale = (CLIP * jnp.sqrt(mean + EPS)).astype(jnp.bfloat16).astype(jnp.float32)
    spread = jnp.broadcast_to(scale[:, None, :], (scale.shape[0], group, TILE)).reshape(values.shape)
    quantized = jnp.clip(values / spread, -1.0, 1.0).astype(jnp.bfloat16)
    result = quantized.astype(jnp.float32) * spread
    decoded[...] = result
    rounded = result.astype(jnp.bfloat16)
    for k in range(sent.shape[0]):
        sent[k] = rounded


def spread_tile(values, offsets):
    rows, width = values.shape
    wide = jnp.broadcast_to(values[:, None, :], (rows, STRIDE, width)).reshape(rows * STRIDE, width)
    return jnp.where(selected(offsets), wide, 0.0)


def inverse_tile(values, offsets, table):
    return right(left(table, spread_tile(values, offsets), 0), table, 0)


def residual_kernel(momentum, summed, decoded, offsets, high, low, out):
    table = (high[...], low[...])
    per = TILE // BLOCK
    rows = TILE // STRIDE
    for i in range(out.shape[0] // TILE):
        here = slice(i * TILE, (i + 1) * TILE)
        value = BETA * momentum[here].astype(jnp.float32) + summed[here].astype(jnp.float32)
        back = inverse_tile(decoded[i * rows : (i + 1) * rows], offsets[i * per : (i + 1) * per], table)
        out[here] = (value - back).astype(jnp.bfloat16)


def update_kernel(parts, offsets, high, low, out):
    table = (high[...], low[...])
    per = TILE // BLOCK
    rows = TILE // STRIDE
    count = parts.shape[0]
    for i in range(out.shape[0] // TILE):
        here = slice(i * rows, (i + 1) * rows)
        total = parts[0, here].astype(jnp.float32)
        for k in range(1, count):
            total += parts[k, here].astype(jnp.float32)
        back = inverse_tile(total * (1.0 / count), offsets[i * per : (i + 1) * per], table)
        out[i * TILE : (i + 1) * TILE] = back.astype(jnp.bfloat16)


def call(kernel, out_shape, flops, scratch=(), in_specs=None, grant=GRANT):
    extra = {} if in_specs is None else {"in_specs": in_specs}
    return pl.pallas_call(
        kernel,
        out_shape=out_shape,
        scratch_shapes=scratch,
        compiler_params=pltpu.CompilerParams(vmem_limit_bytes=grant),
        cost_estimate=pl.CostEstimate(flops=flops, bytes_accessed=2 << 20, transcendentals=0),
        **extra,
    )


def shaped(*shape, dtype=jnp.bfloat16):
    return jax.ShapeDtypeStruct(shape, dtype)


def step(features, out_grads, doc_ids, offsets, momentum):
    shards = lax.axis_size("shard")
    deep = shards // LINES
    groups = lax.axis_size("rep")

    def along_line(x, k):
        pairs = [(y * deep + z, y * deep + (z + k) % deep) for y in range(LINES) for z in range(deep)]
        return lax.ppermute(x, "shard", pairs)

    def across(x, k):
        pairs = [(y * deep + z, (y + k) % LINES * deep + z) for y in range(LINES) for z in range(deep)]
        return lax.ppermute(x, "shard", pairs)

    def exchange(x):
        lines = [[y * deep + z for z in range(deep)] for y in range(LINES)]
        return lax.all_to_all(x, "shard", 0, 0, axis_index_groups=lines, tiled=True)

    rows = features[0, 0]
    grads = out_grads[0, 0]
    tokens, panel = grads.shape
    width = rows.shape[1] // shards
    whole = pl.BlockSpec(memory_space=pltpu.VMEM)
    apart = pl.BlockSpec(memory_space=pltpu.HBM)
    work = 2 * panel * deep * tokens * width

    early = call(
        early_kernel,
        shaped(deep, tokens, panel + width),
        work,
        (pltpu.SemaphoreType.DMA((deep,)),),
        [apart, whole],
        FULL,
    )(rows, grads)
    early = exchange(early)

    onehot = (doc_ids[0, 0][:, None] == jnp.arange(128, dtype=jnp.int32)[None, :]).astype(jnp.float32)
    counts = jnp.broadcast_to(jnp.sum(onehot, axis=0, keepdims=True), (8, 128))
    before = across(counts, 1)
    after = across(counts, -1)
    lanes = jnp.concatenate([counts[:1, :16], before[:1, :16], after[:1, :16]], axis=1)
    extra = jnp.concatenate(
        [onehot[:, :16], jnp.broadcast_to(lanes, (tokens, 48)), jnp.zeros((tokens, 64), jnp.float32)], axis=1
    ).astype(jnp.bfloat16)

    notes = [extra]
    for k in (2, 1, 3):
        notes.append(along_line(extra, k))
    notes = [notes[0], notes[2], notes[1], notes[3]]

    outs = call(
        late_kernel,
        [shaped(tokens, 2 * width)] * deep + [shaped(deep, tokens, 2 * width), shaped(deep, tokens, 3 * width)],
        work,
        (pltpu.SemaphoreType.DMA((7 * deep,)),),
        [apart],
        FULL,
    )(rows)
    third, second, last = list(outs[:deep]), outs[deep], outs[deep + 1]
    for k in (2, 1, 3):
        third[k] = along_line(third[k], k)
    second = exchange(second)
    last = exchange(last)

    weights = call(scale_kernel, shaped(panel, deep * tokens), work)(early, *notes)
    half = panel // 2
    up, down = call(far_kernel, [shaped(half, width)] * 2, work)(weights, early)

    def ring(up, down):
        up = across(up, 1)
        down = across(down, -1)
        return up, down

    def near(start, top, received, parts):
        kernel = functools.partial(near_kernel, start, top, len(parts) > 1)
        return call(kernel, shaped(panel, width), work)(weights, received, *parts)

    up, down = ring(up, down)
    up, down = ring(near(0, True, up, third), near(width, False, down, third))
    up, down = ring(near(0, True, up, [second]), near(width, False, down, [second]))
    up, down = ring(near(0, True, up, [last]), near(width, False, down, [last]))

    high, low = dct_parts()
    ones = jnp.asarray(np.kron(np.eye(TILE // BLOCK), np.ones((BLOCK, BLOCK))), jnp.bfloat16)
    wide = jnp.repeat(offsets[0], BLOCK, axis=1)
    kept = panel // STRIDE
    flops = 6 * 2 * 2 * panel * TILE * TILE
    summed, decoded, sent = call(
        forward_kernel,
        (
            shaped(panel, width),
            shaped(kept, width, dtype=jnp.float32),
            shaped(groups, kept, width),
        ),
        flops,
        (pltpu.VMEM((kept, width), jnp.float32),),
    )(weights, last, up, down, momentum[0], wide, high, low, ones)
    parts = lax.all_to_all(sent, "rep", 0, 0, tiled=True)
    residual = call(residual_kernel, shaped(panel, width), flops)(momentum[0], summed, decoded, wide, high, low)
    update = call(update_kernel, shaped(panel, width), flops)(parts, wide, high, low)
    return residual[None], update[None]


def solution(mesh):
    return jax.shard_map(
        step,
        mesh=mesh,
        in_specs=(
            P(None, "rep", "shard", None),
            P(None, "rep", "shard", None),
            P(None, "rep", "shard"),
            P(None, None, "shard"),
            P("rep", None, "shard"),
        ),
        out_specs=(P("rep", None, "shard"), P(None, None, "shard")),
        check_vma=False,
    )
```

```python
import functools
import math

import jax
import jax.numpy as jnp
import numpy as np
from jax import lax
from jax.experimental import pallas as pl
from jax.experimental.pallas import tpu as pltpu
from jax.sharding import PartitionSpec as P


BLOCK = 64
STRIDE = 16
DOCS = 16
LINES = 8
BETA = 0.9
CLIP = 2.0
EPS = 1e-06


TILE = 256
GRANT = 16 << 20
FULL = 60 << 20


def dct_parts():
    freq = np.arange(BLOCK, dtype=np.float64)[:, None]
    place = np.arange(BLOCK, dtype=np.float64)[None, :]
    table = np.cos(math.pi * (2.0 * place + 1.0) * freq / (2.0 * BLOCK)) * math.sqrt(2.0 / BLOCK)
    table[0] /= math.sqrt(2.0)
    whole = np.kron(np.eye(TILE // BLOCK), table)
    high = whole.astype(jnp.bfloat16)
    low = (whole - high.astype(np.float64)).astype(jnp.bfloat16)
    return jnp.asarray(high), jnp.asarray(low)


def dot(a, b, dims):
    return lax.dot_general(a, b, (dims, ((), ())), preferred_element_type=jnp.float32)


def split(x):
    high = x.astype(jnp.bfloat16)
    return high, (x - high.astype(jnp.float32)).astype(jnp.bfloat16)


def left(table, x, dim):
    (th, tl), (xh, xl) = table, split(x)
    dims = ((dim,), (0,))
    return dot(th, xh, dims) + (dot(th, xl, dims) + dot(tl, xh, dims))


def right(x, table, dim):
    (th, tl), (xh, xl) = table, split(x)
    dims = ((1,), (dim,))
    return dot(xh, th, dims) + (dot(xl, th, dims) + dot(xh, tl, dims))


def selected(offsets):
    count, width = offsets.shape
    shape = (count, BLOCK, width)
    both = lax.broadcasted_iota(jnp.int32, shape, 1) + lax.broadcasted_iota(jnp.int32, shape, 2)
    return ((both & (STRIDE - 1)) == offsets[:, None, :]).reshape(count * BLOCK, width)


def gathered(exchanged, start, size):
    deep = exchanged.shape[0]
    z = lax.axis_index("shard") % deep
    return jnp.concatenate([exchanged[(z - k + deep) % deep, :, start : start + size] for k in range(deep)], axis=0)


def fetch(rows, deep, width, moves, sem):
    me = lax.axis_index("shard")
    line = me // deep
    copies = []
    for i, (owner, z, target) in enumerate(moves):
        block = (line + owner + LINES) % LINES * deep + z
        column = pl.multiple_of(block * width, width)
        copies.append(pltpu.make_async_copy(rows.at[:, pl.ds(column, width)], target, sem.at[i]))
    for copy in copies:
        copy.start()
    return copies


def early_kernel(rows, grads, out, sem):
    deep = out.shape[0]
    panel = grads.shape[1]
    width = out.shape[2] - panel
    moves = [(4, z, out.at[z, :, pl.ds(panel, width)]) for z in range(deep)]
    copies = fetch(rows, deep, width, moves, sem)
    for z in range(deep):
        out[z, :, :panel] = grads[...]
    for copy in copies:
        copy.wait()


def late_kernel(rows, third, second, first, own, sem):
    deep = own.shape[0]
    width = own.shape[2]
    moves = []
    for target, owners in ((third, (3, -3)), (second, (2, -2)), (first, (1, -1)), (own, (0,))):
        for z in range(deep):
            for j, owner in enumerate(owners):
                moves.append((owner, z, target.at[z, :, pl.ds(j * width, width)]))
    for copy in fetch(rows, deep, width, moves, sem):
        copy.wait()


def scale_kernel(exchanged, *rest):
    notes, out = rest[:-1], rest[-1]
    deep, tokens = exchanged.shape[0], exchanged.shape[1]
    panel = out.shape[0]
    z = lax.axis_index("shard") % deep
    marks = [note[...].astype(jnp.float32) for note in notes]
    heads = marks[0][:8]
    for mark in marks[1:]:
        heads = heads + mark[:8]
    lengths = pltpu.roll(heads, 112, 1) + pltpu.roll(heads, 96, 1) + pltpu.roll(heads, 80, 1)
    share = 1.0 / jnp.maximum(lengths[:1], 1.0)
    lane = lax.broadcasted_iota(jnp.int32, (tokens, 128), 1)
    for k in range(deep):
        weight = jnp.sum(jnp.where(lane < DOCS, marks[k] * share, 0.0), axis=1, keepdims=True)
        block = exchanged[(z - k + deep) % deep, :, :panel].astype(jnp.float32)
        out[:, k * tokens : (k + 1) * tokens] = (block * weight).T.astype(jnp.bfloat16)


def far_kernel(weights, exchanged, up, down):
    half = up.shape[0]
    columns = gathered(exchanged, exchanged.shape[2] - up.shape[1], up.shape[1])
    dims = ((1,), (0,))
    up[...] = dot(weights[:half], columns, dims).astype(jnp.bfloat16)
    down[...] = dot(weights[half:], columns, dims).astype(jnp.bfloat16)


def near_kernel(start, top, weights, received, exchanged, out):
    width = out.shape[1]
    total = dot(weights[...], gathered(exchanged, start, width), ((1,), (0,)))
    rows = received.shape[0]
    if rows == out.shape[0]:
        out[...] = (total + received[...].astype(jnp.float32)).astype(jnp.bfloat16)
    else:
        here, other = (slice(0, rows), slice(rows, None)) if top else (slice(rows, None), slice(0, rows))
        out[here] = (total[here] + received[...].astype(jnp.float32)).astype(jnp.bfloat16)
        out[other] = total[other].astype(jnp.bfloat16)


def base_kernel(weights, exchanged, momentum, offsets, *rest):
    tables, (product, kept, offsets_out, *tables_out) = rest[: len(rest) // 2 - 1], rest[len(rest) // 2 - 1 :]
    product[...] = dot(weights[...], gathered(exchanged, 0, product.shape[1]), ((1,), (0,)))
    kept[...] = momentum[...]
    offsets_out[...] = offsets[...]
    for table, out in zip(tables, tables_out):
        out[...] = table[...]


def forward_kernel(product, up, down, momentum, offsets, high, low, ones, summed, decoded, sent, packed, held, sem):
    table = (high[...], low[...])
    per = TILE // BLOCK
    rows = TILE // STRIDE
    copies = []
    for i in range(product.shape[0] // TILE):
        here = slice(i * TILE, (i + 1) * TILE)
        total = product[here] + up[here].astype(jnp.float32) + down[here].astype(jnp.float32)
        gradient = total.astype(jnp.bfloat16)
        held[here] = gradient
        copies.append(pltpu.make_async_copy(held.at[pl.ds(i * TILE, TILE)], summed.at[pl.ds(i * TILE, TILE)], sem.at[i]))
        copies[-1].start()
        value = BETA * momentum[here].astype(jnp.float32) + gradient.astype(jnp.float32)
        spectrum = right(left(table, value, 1), table, 1)
        kept = jnp.where(selected(offsets[i * per : (i + 1) * per]), spectrum, 0.0)
        packed[i * rows : (i + 1) * rows] = jnp.sum(kept.reshape(rows, STRIDE, TILE), axis=1)
    values = packed[...]
    group = BLOCK // STRIDE
    squares = jnp.sum((values * values).reshape(-1, group, TILE), axis=1)
    first = squares.astype(jnp.bfloat16)
    rest = squares - first.astype(jnp.float32)
    second, third = split(rest)
    dims = ((1,), (0,))
    total = dot(first, ones[...], dims) + (dot(second, ones[...], dims) + dot(third, ones[...], dims))
    mean = total * (1.0 / (BLOCK * group))
    scale = (CLIP * jnp.sqrt(mean + EPS)).astype(jnp.bfloat16).astype(jnp.float32)
    spread = jnp.broadcast_to(scale[:, None, :], (scale.shape[0], group, TILE)).reshape(values.shape)
    quantized = jnp.clip(values / spread, -1.0, 1.0).astype(jnp.bfloat16)
    result = quantized.astype(jnp.float32) * spread
    decoded[...] = result
    rounded = result.astype(jnp.bfloat16)
    for k in range(sent.shape[0]):
        sent[k] = rounded
    for copy in copies:
        copy.wait()


def spread_tile(values, offsets):
    rows, width = values.shape
    wide = jnp.broadcast_to(values[:, None, :], (rows, STRIDE, width)).reshape(rows * STRIDE, width)
    return jnp.where(selected(offsets), wide, 0.0)


def inverse_tile(values, offsets, table):
    return right(left(table, spread_tile(values, offsets), 0), table, 0)


def residual_kernel(momentum, summed, decoded, offsets, high, low, out):
    table = (high[...], low[...])
    per = TILE // BLOCK
    rows = TILE // STRIDE
    for i in range(out.shape[0] // TILE):
        here = slice(i * TILE, (i + 1) * TILE)
        value = BETA * momentum[here].astype(jnp.float32) + summed[here].astype(jnp.float32)
        back = inverse_tile(decoded[i * rows : (i + 1) * rows], offsets[i * per : (i + 1) * per], table)
        out[here] = (value - back).astype(jnp.bfloat16)


def update_kernel(parts, offsets, high, low, out):
    table = (high[...], low[...])
    per = TILE // BLOCK
    rows = TILE // STRIDE
    count = parts.shape[0]
    for i in range(out.shape[0] // TILE):
        here = slice(i * rows, (i + 1) * rows)
        total = parts[0, here].astype(jnp.float32)
        for k in range(1, count):
            total += parts[k, here].astype(jnp.float32)
        back = inverse_tile(total * (1.0 / count), offsets[i * per : (i + 1) * per], table)
        out[i * TILE : (i + 1) * TILE] = back.astype(jnp.bfloat16)


def call(kernel, out_shape, flops, scratch=(), in_specs=None, grant=GRANT):
    extra = {} if in_specs is None else {"in_specs": in_specs}
    return pl.pallas_call(
        kernel,
        out_shape=out_shape,
        scratch_shapes=scratch,
        compiler_params=pltpu.CompilerParams(vmem_limit_bytes=grant),
        cost_estimate=pl.CostEstimate(flops=flops, bytes_accessed=2 << 20, transcendentals=0),
        **extra,
    )


def shaped(*shape, dtype=jnp.bfloat16):
    return jax.ShapeDtypeStruct(shape, dtype)


def step(features, out_grads, doc_ids, offsets, momentum):
    shards = lax.axis_size("shard")
    deep = shards // LINES
    groups = lax.axis_size("rep")

    def along_line(x, k):
        pairs = [(y * deep + z, y * deep + (z + k) % deep) for y in range(LINES) for z in range(deep)]
        return lax.ppermute(x, "shard", pairs)

    def across(x, k):
        pairs = [(y * deep + z, (y + k) % LINES * deep + z) for y in range(LINES) for z in range(deep)]
        return lax.ppermute(x, "shard", pairs)

    def exchange(x):
        lines = [[y * deep + z for z in range(deep)] for y in range(LINES)]
        return lax.all_to_all(x, "shard", 0, 0, axis_index_groups=lines, tiled=True)

    rows = features[0, 0]
    grads = out_grads[0, 0]
    tokens, panel = grads.shape
    width = rows.shape[1] // shards
    whole = pl.BlockSpec(memory_space=pltpu.VMEM)
    apart = pl.BlockSpec(memory_space=pltpu.HBM)
    work = 2 * panel * deep * tokens * width

    early = call(
        early_kernel,
        shaped(deep, tokens, panel + width),
        work,
        (pltpu.SemaphoreType.DMA((deep,)),),
        [apart, whole],
        FULL,
    )(rows, grads)
    early = exchange(early)

    onehot = (doc_ids[0, 0][:, None] == jnp.arange(128, dtype=jnp.int32)[None, :]).astype(jnp.float32)
    counts = jnp.broadcast_to(jnp.sum(onehot, axis=0, keepdims=True), (8, 128))
    before = across(counts, 1)
    after = across(counts, -1)
    lanes = jnp.concatenate([counts[:1, :16], before[:1, :16], after[:1, :16]], axis=1)
    extra = jnp.concatenate(
        [onehot[:, :16], jnp.broadcast_to(lanes, (tokens, 48)), jnp.zeros((tokens, 64), jnp.float32)], axis=1
    ).astype(jnp.bfloat16)

    notes = [extra]
    for k in (2, 1, 3):
        notes.append(along_line(extra, k))
    notes = [notes[0], notes[2], notes[1], notes[3]]

    third, second, first, own = call(
        late_kernel,
        [shaped(deep, tokens, 2 * width)] * 3 + [shaped(deep, tokens, width)],
        work,
        (pltpu.SemaphoreType.DMA((7 * deep,)),),
        [apart],
        FULL,
    )(rows)
    third = exchange(third)
    second = exchange(second)
    first = exchange(first)
    own = exchange(own)

    weights = call(scale_kernel, shaped(panel, deep * tokens), work)(early, *notes)
    half = panel // 2
    up, down = call(far_kernel, [shaped(half, width)] * 2, work)(weights, early)

    def ring(up, down):
        up = across(up, 1)
        down = across(down, -1)
        return up, down

    def near(start, top, received, exchanged):
        kernel = functools.partial(near_kernel, start, top)
        return call(kernel, shaped(panel, width), work)(weights, received, exchanged)

    def both(up, down, exchanged):
        return near(0, True, up, exchanged), near(width, False, down, exchanged)

    up, down = ring(up, down)
    up, down = ring(*both(up, down, third))
    up, down = ring(*both(up, down, second))
    up, down = ring(*both(up, down, first))

    high, low = dct_parts()
    ones = jnp.asarray(np.kron(np.eye(TILE // BLOCK), np.ones((BLOCK, BLOCK))), jnp.bfloat16)
    wide = jnp.repeat(offsets[0], BLOCK, axis=1)
    kept = panel // STRIDE
    flops = 6 * 2 * 2 * panel * TILE * TILE
    tables = (high, low, ones)
    product, momentum_near, wide_near, *tables_near = call(
        base_kernel,
        [shaped(panel, width, dtype=jnp.float32), shaped(panel, width), shaped(*wide.shape, dtype=jnp.int32)]
        + [shaped(*table.shape) for table in tables],
        work,
    )(weights, own, momentum[0], wide, *tables)
    summed, decoded, sent = pl.pallas_call(
        forward_kernel,
        out_shape=(shaped(panel, width), shaped(kept, width, dtype=jnp.float32), shaped(groups, kept, width)),
        out_specs=(apart, whole, whole),
        scratch_shapes=(
            pltpu.VMEM((kept, width), jnp.float32),
            pltpu.VMEM((panel, width), jnp.bfloat16),
            pltpu.SemaphoreType.DMA((panel // TILE,)),
        ),
        compiler_params=pltpu.CompilerParams(vmem_limit_bytes=GRANT),
        cost_estimate=pl.CostEstimate(flops=flops, bytes_accessed=2 << 20, transcendentals=0),
    )(product, up, down, momentum_near, wide_near, *tables_near)
    parts = lax.all_to_all(sent, "rep", 0, 0, tiled=True)
    residual = call(residual_kernel, shaped(panel, width), flops)(momentum[0], summed, decoded, wide, high, low)
    update = call(update_kernel, shaped(panel, width), flops)(parts, wide, high, low)
    return residual[None], update[None]


def solution(mesh):
    return jax.shard_map(
        step,
        mesh=mesh,
        in_specs=(
            P(None, "rep", "shard", None),
            P(None, "rep", "shard", None),
            P(None, "rep", "shard"),
            P(None, None, "shard"),
            P("rep", None, "shard"),
        ),
        out_specs=(P("rep", None, "shard"), P(None, None, "shard")),
        check_vma=False,
    )
```

```python
import functools
import math

import jax
import jax.numpy as jnp
import numpy as np
from jax import lax
from jax.experimental import pallas as pl
from jax.experimental.pallas import tpu as pltpu
from jax.sharding import PartitionSpec as P


BLOCK = 64
STRIDE = 16
DOCS = 16
LINES = 8
BETA = 0.9
CLIP = 2.0
EPS = 1e-06


TILE = 256
GRANT = 16 << 20
FULL = 60 << 20


def dct_parts():
    freq = np.arange(BLOCK, dtype=np.float64)[:, None]
    place = np.arange(BLOCK, dtype=np.float64)[None, :]
    table = np.cos(math.pi * (2.0 * place + 1.0) * freq / (2.0 * BLOCK)) * math.sqrt(2.0 / BLOCK)
    table[0] /= math.sqrt(2.0)
    whole = np.kron(np.eye(TILE // BLOCK), table)
    high = whole.astype(jnp.bfloat16)
    low = (whole - high.astype(np.float64)).astype(jnp.bfloat16)
    some = slice(0, BLOCK)
    ahead = np.concatenate([high[some, some], high[some, some], low[some, some]], axis=1)
    back = np.concatenate([high[some, some].T, high[some, some].T, low[some, some].T], axis=1)
    return tuple(jnp.asarray(part) for part in (high, low, ahead, back))


def dot(a, b, dims):
    return lax.dot_general(a, b, (dims, ((), ())), preferred_element_type=jnp.float32)


def split(x):
    high = x.astype(jnp.bfloat16)
    return high, (x - high.astype(jnp.float32)).astype(jnp.bfloat16)


def left(table, x):
    high, low = split(x)
    dims = ((1,), (0,))
    out = []
    for i in range(x.shape[0] // BLOCK):
        here = slice(i * BLOCK, (i + 1) * BLOCK)
        out.append(dot(table, jnp.concatenate([high[here], low[here], high[here]], axis=0), dims))
    return jnp.concatenate(out, axis=0)


def right(x, table, dim):
    (th, tl), (xh, xl) = table, split(x)
    dims = ((1,), (dim,))
    return dot(xh, th, dims) + (dot(xl, th, dims) + dot(xh, tl, dims))


def selected(offsets):
    count, width = offsets.shape
    shape = (count, BLOCK, width)
    both = lax.broadcasted_iota(jnp.int32, shape, 1) + lax.broadcasted_iota(jnp.int32, shape, 2)
    return ((both & (STRIDE - 1)) == offsets[:, None, :]).reshape(count * BLOCK, width)


def gathered(exchanged, start, size):
    deep = exchanged.shape[0]
    z = lax.axis_index("shard") % deep
    return jnp.concatenate([exchanged[(z - k + deep) % deep, :, start : start + size] for k in range(deep)], axis=0)


def fetch(rows, deep, width, moves, sem):
    me = lax.axis_index("shard")
    line = me // deep
    copies = []
    for i, (owner, z, target) in enumerate(moves):
        block = (line + owner + LINES) % LINES * deep + z
        column = pl.multiple_of(block * width, width)
        copies.append(pltpu.make_async_copy(rows.at[:, pl.ds(column, width)], target, sem.at[i]))
    for copy in copies:
        copy.start()
    return copies


def early_kernel(rows, grads, out, sem, given):
    deep = out.shape[0]
    panel = grads.shape[1]
    width = out.shape[2] - panel
    moves = [(4, z, out.at[z, :, pl.ds(panel, width)]) for z in range(deep)]
    copies = fetch(rows, deep, width, moves, sem)
    for z in range(deep):
        copies.append(pltpu.make_async_copy(grads, out.at[z, :, pl.ds(0, panel)], given.at[z]))
        copies[-1].start()
    for copy in copies:
        copy.wait()


def late_kernel(rows, third, second, first, sem):
    deep = third.shape[0]
    width = third.shape[2] // 2
    moves = []
    for target, owners in ((third, (3, -3)), (second, (2, -2)), (first, (1, -1, 0))):
        for z in range(deep):
            for j, owner in enumerate(owners):
                moves.append((owner, z, target.at[z, :, pl.ds(j * width, width)]))
    for copy in fetch(rows, deep, width, moves, sem):
        copy.wait()


def scale_kernel(exchanged, *rest):
    notes, out = rest[:-1], rest[-1]
    deep, tokens = exchanged.shape[0], exchanged.shape[1]
    panel = out.shape[0]
    z = lax.axis_index("shard") % deep
    marks = [note[...].astype(jnp.float32) for note in notes]
    heads = marks[0][DOCS:]
    for mark in marks[1:]:
        heads = heads + mark[DOCS:]
    share = 1.0 / jnp.maximum(jnp.sum(heads, axis=1, keepdims=True), 1.0)
    for k in range(deep):
        weight = jnp.sum(marks[k][:DOCS] * share, axis=0, keepdims=True)
        block = exchanged[(z - k + deep) % deep, :, :panel].astype(jnp.float32)
        out[:, k * tokens : (k + 1) * tokens] = (block.T * weight).astype(jnp.bfloat16)


def far_kernel(weights, exchanged, up, down):
    half = up.shape[0]
    columns = gathered(exchanged, exchanged.shape[2] - up.shape[1], up.shape[1])
    dims = ((1,), (0,))
    up[...] = dot(weights[:half], columns, dims).astype(jnp.bfloat16)
    down[...] = dot(weights[half:], columns, dims).astype(jnp.bfloat16)


def near_kernel(start, top, weights, received, exchanged, out):
    width = out.shape[1]
    total = dot(weights[...], gathered(exchanged, start, width), ((1,), (0,)))
    rows = received.shape[0]
    if rows == out.shape[0]:
        out[...] = (total + received[...].astype(jnp.float32)).astype(jnp.bfloat16)
    else:
        here, other = (slice(0, rows), slice(rows, None)) if top else (slice(rows, None), slice(0, rows))
        out[here] = (total[here] + received[...].astype(jnp.float32)).astype(jnp.bfloat16)
        out[other] = total[other].astype(jnp.bfloat16)


def base_kernel(weights, exchanged, momentum, offsets, *rest):
    tables, (product, kept, offsets_out, *tables_out) = rest[: len(rest) // 2 - 1], rest[len(rest) // 2 - 1 :]
    product[...] = dot(weights[...], gathered(exchanged, 2 * product.shape[1], product.shape[1]), ((1,), (0,)))
    kept[...] = momentum[...]
    offsets_out[...] = offsets[...]
    for table, out in zip(tables, tables_out):
        out[...] = table[...]


def forward_kernel(product, up, down, momentum, offsets, high, low, ahead, ones, summed, decoded, sent, packed, held, sem):
    table = (high[...], low[...])
    per = TILE // BLOCK
    rows = TILE // STRIDE
    copies = []
    for i in range(product.shape[0] // TILE):
        here = slice(i * TILE, (i + 1) * TILE)
        total = product[here] + up[here].astype(jnp.float32) + down[here].astype(jnp.float32)
        gradient = total.astype(jnp.bfloat16)
        held[here] = gradient
        copies.append(pltpu.make_async_copy(held.at[pl.ds(i * TILE, TILE)], summed.at[pl.ds(i * TILE, TILE)], sem.at[i]))
        copies[-1].start()
        value = BETA * momentum[here].astype(jnp.float32) + gradient.astype(jnp.float32)
        spectrum = right(left(ahead[...], value), table, 1)
        kept = jnp.where(selected(offsets[i * per : (i + 1) * per]), spectrum, 0.0)
        packed[i * rows : (i + 1) * rows] = jnp.sum(kept.reshape(rows, STRIDE, TILE), axis=1)
    values = packed[...]
    group = BLOCK // STRIDE
    squares = jnp.sum((values * values).reshape(-1, group, TILE), axis=1)
    first = squares.astype(jnp.bfloat16)
    rest = squares - first.astype(jnp.float32)
    second, third = split(rest)
    dims = ((1,), (0,))
    total = dot(first, ones[...], dims) + (dot(second, ones[...], dims) + dot(third, ones[...], dims))
    mean = total * (1.0 / (BLOCK * group))
    scale = (CLIP * jnp.sqrt(mean + EPS)).astype(jnp.bfloat16).astype(jnp.float32)
    spread = jnp.broadcast_to(scale[:, None, :], (scale.shape[0], group, TILE)).reshape(values.shape)
    quantized = jnp.clip(values / spread, -1.0, 1.0).astype(jnp.bfloat16)
    result = quantized.astype(jnp.float32) * spread
    decoded[...] = result
    rounded = result.astype(jnp.bfloat16)
    for k in range(sent.shape[0]):
        sent[k] = rounded
    for copy in copies:
        copy.wait()


def spread_tile(values, offsets):
    rows, width = values.shape
    wide = jnp.broadcast_to(values[:, None, :], (rows, STRIDE, width)).reshape(rows * STRIDE, width)
    return jnp.where(selected(offsets), wide, 0.0)


def inverse_tile(values, offsets, table, back):
    return right(left(back, spread_tile(values, offsets)), table, 0)


def residual_kernel(momentum, summed, decoded, offsets, high, low, back_table, out):
    table = (high[...], low[...])
    per = TILE // BLOCK
    rows = TILE // STRIDE
    for i in range(out.shape[0] // TILE):
        here = slice(i * TILE, (i + 1) * TILE)
        value = BETA * momentum[here].astype(jnp.float32) + summed[here].astype(jnp.float32)
        back = inverse_tile(decoded[i * rows : (i + 1) * rows], offsets[i * per : (i + 1) * per], table, back_table[...])
        out[here] = (value - back).astype(jnp.bfloat16)


def update_kernel(parts, offsets, high, low, back_table, out):
    table = (high[...], low[...])
    per = TILE // BLOCK
    rows = TILE // STRIDE
    count = parts.shape[0]
    for i in range(out.shape[0] // TILE):
        here = slice(i * rows, (i + 1) * rows)
        total = parts[0, here].astype(jnp.float32)
        for k in range(1, count):
            total += parts[k, here].astype(jnp.float32)
        back = inverse_tile(total * (1.0 / count), offsets[i * per : (i + 1) * per], table, back_table[...])
        out[i * TILE : (i + 1) * TILE] = back.astype(jnp.bfloat16)


def call(kernel, out_shape, flops, scratch=(), in_specs=None, grant=GRANT):
    extra = {} if in_specs is None else {"in_specs": in_specs}
    return pl.pallas_call(
        kernel,
        out_shape=out_shape,
        scratch_shapes=scratch,
        compiler_params=pltpu.CompilerParams(vmem_limit_bytes=grant),
        cost_estimate=pl.CostEstimate(flops=flops, bytes_accessed=2 << 20, transcendentals=0),
        **extra,
    )


def shaped(*shape, dtype=jnp.bfloat16):
    return jax.ShapeDtypeStruct(shape, dtype)


def step(features, out_grads, doc_ids, offsets, momentum):
    shards = lax.axis_size("shard")
    deep = shards // LINES
    groups = lax.axis_size("rep")

    def along_line(x, k):
        pairs = [(y * deep + z, y * deep + (z + k) % deep) for y in range(LINES) for z in range(deep)]
        return lax.ppermute(x, "shard", pairs)

    def across(x, k):
        pairs = [(y * deep + z, (y + k) % LINES * deep + z) for y in range(LINES) for z in range(deep)]
        return lax.ppermute(x, "shard", pairs)

    def exchange(x):
        lines = [[y * deep + z for z in range(deep)] for y in range(LINES)]
        return lax.all_to_all(x, "shard", 0, 0, axis_index_groups=lines, tiled=True)

    rows = features[0, 0]
    grads = out_grads[0, 0]
    tokens, panel = grads.shape
    width = rows.shape[1] // shards
    whole = pl.BlockSpec(memory_space=pltpu.VMEM)
    apart = pl.BlockSpec(memory_space=pltpu.HBM)
    work = 2 * panel * deep * tokens * width

    early = call(
        early_kernel,
        shaped(deep, tokens, panel + width),
        work,
        (pltpu.SemaphoreType.DMA((deep,)), pltpu.SemaphoreType.DMA((deep,))),
        [apart, apart],
        FULL,
    )(rows, grads)
    early = exchange(early)

    documents = lax.broadcasted_iota(jnp.int32, (DOCS, tokens), 0)
    onehot = (doc_ids[0] == documents).astype(jnp.float32)
    counts = jnp.broadcast_to(jnp.sum(onehot, axis=1, keepdims=True), (DOCS, tokens))
    before = across(counts, 1)
    after = across(counts, -1)
    lane = lax.broadcasted_iota(jnp.int32, (DOCS, tokens), 1)
    heads = jnp.where(lane == 0, counts, jnp.where(lane == 1, before, jnp.where(lane == 2, after, 0.0)))
    extra = jnp.concatenate([onehot, heads], axis=0).astype(jnp.bfloat16)

    notes = [extra]
    for k in (2, 1, 3):
        notes.append(along_line(extra, k))
    notes = [notes[0], notes[2], notes[1], notes[3]]

    third, second, first = call(
        late_kernel,
        [shaped(deep, tokens, 2 * width)] * 2 + [shaped(deep, tokens, 3 * width)],
        work,
        (pltpu.SemaphoreType.DMA((7 * deep,)),),
        [apart],
        FULL,
    )(rows)
    third = exchange(third)
    second = exchange(second)
    first = exchange(first)

    weights = call(scale_kernel, shaped(panel, deep * tokens), work)(early, *notes)
    half = panel // 2
    up, down = call(far_kernel, [shaped(half, width)] * 2, work)(weights, early)

    def ring(up, down):
        up = across(up, 1)
        down = across(down, -1)
        return up, down

    def near(start, top, received, exchanged):
        kernel = functools.partial(near_kernel, start, top)
        return call(kernel, shaped(panel, width), work)(weights, received, exchanged)

    def both(up, down, exchanged):
        return near(0, True, up, exchanged), near(width, False, down, exchanged)

    up, down = ring(up, down)
    up, down = ring(*both(up, down, third))
    up, down = ring(*both(up, down, second))
    up, down = ring(*both(up, down, first))

    high, low, ahead, back = dct_parts()
    ones = jnp.asarray(np.kron(np.eye(TILE // BLOCK), np.ones((BLOCK, BLOCK))), jnp.bfloat16)
    wide = jnp.repeat(offsets[0], BLOCK, axis=1)
    kept = panel // STRIDE
    flops = 6 * 2 * 2 * panel * TILE * TILE
    tables = (high, low, ahead, ones)
    product, momentum_near, wide_near, *tables_near = call(
        base_kernel,
        [shaped(panel, width, dtype=jnp.float32), shaped(panel, width), shaped(*wide.shape, dtype=jnp.int32)]
        + [shaped(*table.shape) for table in tables],
        work,
    )(weights, first, momentum[0], wide, *tables)
    summed, decoded, sent = pl.pallas_call(
        forward_kernel,
        out_shape=(shaped(panel, width), shaped(kept, width, dtype=jnp.float32), shaped(groups, kept, width)),
        out_specs=(apart, whole, whole),
        scratch_shapes=(
            pltpu.VMEM((kept, width), jnp.float32),
            pltpu.VMEM((panel, width), jnp.bfloat16),
            pltpu.SemaphoreType.DMA((panel // TILE,)),
        ),
        compiler_params=pltpu.CompilerParams(vmem_limit_bytes=GRANT),
        cost_estimate=pl.CostEstimate(flops=flops, bytes_accessed=2 << 20, transcendentals=0),
    )(product, up, down, momentum_near, wide_near, *tables_near)
    parts = lax.all_to_all(sent, "rep", 0, 0, tiled=True)
    residual = call(residual_kernel, shaped(panel, width), flops)(momentum[0], summed, decoded, wide, high, low, back)
    update = call(update_kernel, shaped(panel, width), flops)(parts, wide, high, low, back)
    return residual[None], update[None]


def solution(mesh):
    return jax.shard_map(
        step,
        mesh=mesh,
        in_specs=(
            P(None, "rep", "shard", None),
            P(None, "rep", "shard", None),
            P(None, "rep", "shard"),
            P(None, None, "shard"),
            P("rep", None, "shard"),
        ),
        out_specs=(P("rep", None, "shard"), P(None, None, "shard")),
        check_vma=False,
    )
```

```python
import functools
import math

import jax
import jax.numpy as jnp
import numpy as np
from jax import lax
from jax.experimental import pallas as pl
from jax.experimental.pallas import tpu as pltpu
from jax.sharding import PartitionSpec as P


BLOCK = 64
STRIDE = 16
DOCS = 16
LINES = 8
BETA = 0.9
CLIP = 2.0
EPS = 1e-06


TILE = 256
GRANT = 16 << 20
NOTE_ROWS = 8
FULL = 60 << 20


def dct_parts():
    freq = np.arange(BLOCK, dtype=np.float64)[:, None]
    place = np.arange(BLOCK, dtype=np.float64)[None, :]
    table = np.cos(math.pi * (2.0 * place + 1.0) * freq / (2.0 * BLOCK)) * math.sqrt(2.0 / BLOCK)
    table[0] /= math.sqrt(2.0)
    whole = np.kron(np.eye(TILE // BLOCK), table)
    high = whole.astype(jnp.bfloat16)
    low = (whole - high.astype(np.float64)).astype(jnp.bfloat16)
    some = slice(0, BLOCK)
    ahead = np.concatenate([high[some, some], high[some, some], low[some, some]], axis=1)
    back = np.concatenate([high[some, some].T, high[some, some].T, low[some, some].T], axis=1)
    return tuple(jnp.asarray(part) for part in (high, low, ahead, back))


def dot(a, b, dims):
    return lax.dot_general(a, b, (dims, ((), ())), preferred_element_type=jnp.float32)


def split(x):
    high = x.astype(jnp.bfloat16)
    return high, (x - high.astype(jnp.float32)).astype(jnp.bfloat16)


def left(table, x):
    high, low = split(x)
    dims = ((1,), (0,))
    out = []
    for i in range(x.shape[0] // BLOCK):
        here = slice(i * BLOCK, (i + 1) * BLOCK)
        out.append(dot(table, jnp.concatenate([high[here], low[here], high[here]], axis=0), dims))
    return jnp.concatenate(out, axis=0)


def right(x, table, dim):
    (th, tl), (xh, xl) = table, split(x)
    dims = ((1,), (dim,))
    return dot(xh, th, dims) + (dot(xl, th, dims) + dot(xh, tl, dims))


def selected(offsets):
    count, width = offsets.shape
    shape = (count, BLOCK, width)
    both = lax.broadcasted_iota(jnp.int32, shape, 1) + lax.broadcasted_iota(jnp.int32, shape, 2)
    return ((both & (STRIDE - 1)) == offsets[:, None, :]).reshape(count * BLOCK, width)


def gathered(exchanged, start, size):
    deep = exchanged.shape[0]
    tokens = exchanged.shape[1] // 128 * 128
    z = lax.axis_index("shard") % deep
    return jnp.concatenate([exchanged[(z - k + deep) % deep, :tokens, start : start + size] for k in range(deep)], axis=0)


def fetch(rows, deep, width, moves, sem):
    me = lax.axis_index("shard")
    line = me // deep
    copies = []
    for i, (owner, z, target) in enumerate(moves):
        block = (line + owner + LINES) % LINES * deep + z
        column = pl.multiple_of(block * width, width)
        copies.append(pltpu.make_async_copy(rows.at[:, pl.ds(column, width)], target, sem.at[i]))
    for copy in copies:
        copy.start()
    return copies


def early_kernel(rows, grads, ids, out, sem, given):
    deep = out.shape[0]
    tokens, panel = grads.shape
    width = out.shape[2] - panel
    here = pl.ds(0, tokens)
    moves = [(4, z, out.at[z, here, pl.ds(panel, width)]) for z in range(deep)]
    copies = fetch(rows, deep, width, moves, sem)
    for z in range(deep):
        copies.append(pltpu.make_async_copy(grads, out.at[z, here, pl.ds(0, panel)], given.at[z]))
        copies[-1].start()
    for z in range(deep):
        out[z, tokens:, :tokens] = jnp.broadcast_to(ids[...], (NOTE_ROWS, tokens)).astype(jnp.bfloat16)
    for copy in copies:
        copy.wait()


def late_kernel(rows, third, second, first, sem):
    deep = third.shape[0]
    width = third.shape[2] // 2
    moves = []
    for target, owners in ((third, (3, -3)), (second, (2, -2)), (first, (1, -1, 0))):
        for z in range(deep):
            for j, owner in enumerate(owners):
                moves.append((owner, z, target.at[z, :, pl.ds(j * width, width)]))
    for copy in fetch(rows, deep, width, moves, sem):
        copy.wait()


def marked(exchanged, k):
    deep = exchanged.shape[0]
    tokens = exchanged.shape[1] - NOTE_ROWS
    z = lax.axis_index("shard") % deep
    ids = exchanged[(z - k + deep) % deep, tokens:, :tokens].astype(jnp.float32)[:1]
    documents = lax.broadcasted_iota(jnp.int32, (DOCS, tokens), 0).astype(jnp.float32)
    return jnp.where(ids == documents, 1.0, 0.0)


def count_kernel(exchanged, out):
    total = sum(marked(exchanged, k) for k in range(exchanged.shape[0]))
    out[...] = jnp.broadcast_to(jnp.sum(total, axis=1, keepdims=True), out.shape)


def scale_kernel(exchanged, counts, before, after, out):
    deep = exchanged.shape[0]
    tokens = exchanged.shape[1] - NOTE_ROWS
    panel = out.shape[0]
    z = lax.axis_index("shard") % deep
    share = 1.0 / jnp.maximum(counts[...] + before[...] + after[...], 1.0)
    for k in range(deep):
        weight = jnp.sum(marked(exchanged, k) * share, axis=0, keepdims=True)
        block = exchanged[(z - k + deep) % deep, :tokens, :panel].astype(jnp.float32)
        out[:, k * tokens : (k + 1) * tokens] = (block.T * weight).astype(jnp.bfloat16)


def far_kernel(weights, exchanged, up, down):
    half = up.shape[0]
    columns = gathered(exchanged, exchanged.shape[2] - up.shape[1], up.shape[1])
    dims = ((1,), (0,))
    up[...] = dot(weights[:half], columns, dims).astype(jnp.bfloat16)
    down[...] = dot(weights[half:], columns, dims).astype(jnp.bfloat16)


def near_kernel(start, top, weights, received, exchanged, out):
    width = out.shape[1]
    total = dot(weights[...], gathered(exchanged, start, width), ((1,), (0,)))
    rows = received.shape[0]
    if rows == out.shape[0]:
        out[...] = (total + received[...].astype(jnp.float32)).astype(jnp.bfloat16)
    else:
        here, other = (slice(0, rows), slice(rows, None)) if top else (slice(rows, None), slice(0, rows))
        out[here] = (total[here] + received[...].astype(jnp.float32)).astype(jnp.bfloat16)
        out[other] = total[other].astype(jnp.bfloat16)


def base_kernel(weights, exchanged, momentum, offsets, *rest):
    tables, (product, kept, offsets_out, *tables_out) = rest[: len(rest) // 2 - 1], rest[len(rest) // 2 - 1 :]
    product[...] = dot(weights[...], gathered(exchanged, 2 * product.shape[1], product.shape[1]), ((1,), (0,)))
    kept[...] = momentum[...]
    offsets_out[...] = offsets[...]
    for table, out in zip(tables, tables_out):
        out[...] = table[...]


def forward_kernel(
    product, up, down, momentum, offsets, high, low, ahead, ones, summed, decoded, sent, packed, held, parts, sem
):
    table = (high[...], low[...])
    per = TILE // BLOCK
    rows = TILE // STRIDE
    fetches = []
    for i in range(product.shape[0] // TILE):
        there = pl.ds(i * TILE, TILE)
        pair = [pltpu.make_async_copy(x.at[there], parts.at[j, there], sem.at[1 + j, i]) for j, x in enumerate((up, down))]
        fetches.append(pair)
        for copy in pair:
            copy.start()
    copies = []
    for i in range(product.shape[0] // TILE):
        here = slice(i * TILE, (i + 1) * TILE)
        for copy in fetches[i]:
            copy.wait()
        total = product[here] + parts[0, here].astype(jnp.float32) + parts[1, here].astype(jnp.float32)
        gradient = total.astype(jnp.bfloat16)
        held[here] = gradient
        copies.append(pltpu.make_async_copy(held.at[pl.ds(i * TILE, TILE)], summed.at[pl.ds(i * TILE, TILE)], sem.at[0, i]))
        copies[-1].start()
        value = BETA * momentum[here].astype(jnp.float32) + gradient.astype(jnp.float32)
        spectrum = right(left(ahead[...], value), table, 1)
        kept = jnp.where(selected(offsets[i * per : (i + 1) * per]), spectrum, 0.0)
        packed[i * rows : (i + 1) * rows] = jnp.sum(kept.reshape(rows, STRIDE, TILE), axis=1)
    values = packed[...]
    group = BLOCK // STRIDE
    squares = jnp.sum((values * values).reshape(-1, group, TILE), axis=1)
    first = squares.astype(jnp.bfloat16)
    rest = squares - first.astype(jnp.float32)
    second, third = split(rest)
    dims = ((1,), (0,))
    total = dot(first, ones[...], dims) + (dot(second, ones[...], dims) + dot(third, ones[...], dims))
    mean = total * (1.0 / (BLOCK * group))
    scale = (CLIP * jnp.sqrt(mean + EPS)).astype(jnp.bfloat16).astype(jnp.float32)
    spread = jnp.broadcast_to(scale[:, None, :], (scale.shape[0], group, TILE)).reshape(values.shape)
    quantized = jnp.clip(values / spread, -1.0, 1.0).astype(jnp.bfloat16)
    result = quantized.astype(jnp.float32) * spread
    decoded[...] = result
    rounded = result.astype(jnp.bfloat16)
    for k in range(sent.shape[0]):
        sent[k] = rounded
    for copy in copies:
        copy.wait()


def spread_tile(values, offsets):
    rows, width = values.shape
    wide = jnp.broadcast_to(values[:, None, :], (rows, STRIDE, width)).reshape(rows * STRIDE, width)
    return jnp.where(selected(offsets), wide, 0.0)


def inverse_tile(values, offsets, table, back):
    return right(left(back, spread_tile(values, offsets)), table, 0)


def residual_kernel(momentum, summed, decoded, offsets, high, low, back_table, out):
    table = (high[...], low[...])
    per = TILE // BLOCK
    rows = TILE // STRIDE
    for i in range(out.shape[0] // TILE):
        here = slice(i * TILE, (i + 1) * TILE)
        value = BETA * momentum[here].astype(jnp.float32) + summed[here].astype(jnp.float32)
        back = inverse_tile(decoded[i * rows : (i + 1) * rows], offsets[i * per : (i + 1) * per], table, back_table[...])
        out[here] = (value - back).astype(jnp.bfloat16)


def update_kernel(parts, offsets, high, low, back_table, out):
    table = (high[...], low[...])
    per = TILE // BLOCK
    rows = TILE // STRIDE
    count = parts.shape[0]
    for i in range(out.shape[0] // TILE):
        here = slice(i * rows, (i + 1) * rows)
        total = parts[0, here].astype(jnp.float32)
        for k in range(1, count):
            total += parts[k, here].astype(jnp.float32)
        back = inverse_tile(total * (1.0 / count), offsets[i * per : (i + 1) * per], table, back_table[...])
        out[i * TILE : (i + 1) * TILE] = back.astype(jnp.bfloat16)


def call(kernel, out_shape, flops, scratch=(), in_specs=None, grant=GRANT):
    extra = {} if in_specs is None else {"in_specs": in_specs}
    return pl.pallas_call(
        kernel,
        out_shape=out_shape,
        scratch_shapes=scratch,
        compiler_params=pltpu.CompilerParams(vmem_limit_bytes=grant),
        cost_estimate=pl.CostEstimate(flops=flops, bytes_accessed=2 << 20, transcendentals=0),
        **extra,
    )


def shaped(*shape, dtype=jnp.bfloat16):
    return jax.ShapeDtypeStruct(shape, dtype)


def step(features, out_grads, doc_ids, offsets, momentum):
    shards = lax.axis_size("shard")
    deep = shards // LINES
    groups = lax.axis_size("rep")

    def across(x, k):
        pairs = [(y * deep + z, (y + k) % LINES * deep + z) for y in range(LINES) for z in range(deep)]
        return lax.ppermute(x, "shard", pairs)

    def exchange(x):
        lines = [[y * deep + z for z in range(deep)] for y in range(LINES)]
        return lax.all_to_all(x, "shard", 0, 0, axis_index_groups=lines, tiled=True)

    rows = features[0, 0]
    grads = out_grads[0, 0]
    tokens, panel = grads.shape
    width = rows.shape[1] // shards
    whole = pl.BlockSpec(memory_space=pltpu.VMEM)
    apart = pl.BlockSpec(memory_space=pltpu.HBM)
    work = 2 * panel * deep * tokens * width

    early = call(
        early_kernel,
        shaped(deep, tokens + NOTE_ROWS, panel + width),
        work,
        (pltpu.SemaphoreType.DMA((deep,)), pltpu.SemaphoreType.DMA((deep,))),
        [apart, apart, whole],
        FULL,
    )(rows, grads, doc_ids[0].astype(jnp.float32))
    early = exchange(early)

    third, second, first = call(
        late_kernel,
        [shaped(deep, tokens, 2 * width)] * 2 + [shaped(deep, tokens, 3 * width)],
        work,
        (pltpu.SemaphoreType.DMA((7 * deep,)),),
        [apart],
        FULL,
    )(rows)
    third = exchange(third)
    second = exchange(second)
    first = exchange(first)

    counts = call(count_kernel, shaped(DOCS, 128, dtype=jnp.float32), work // 64)(early)
    before = across(counts, 1)
    after = across(counts, -1)
    weights = call(scale_kernel, shaped(panel, deep * tokens), work)(early, counts, before, after)
    half = panel // 2
    up, down = call(far_kernel, [shaped(half, width)] * 2, work)(weights, early)

    def ring(up, down):
        up = across(up, 1)
        down = across(down, -1)
        return up, down

    def near(start, top, received, exchanged):
        kernel = functools.partial(near_kernel, start, top)
        return call(kernel, shaped(panel, width), work)(weights, received, exchanged)

    def both(up, down, exchanged):
        return near(0, True, up, exchanged), near(width, False, down, exchanged)

    up, down = ring(up, down)
    up, down = ring(*both(up, down, third))
    up, down = ring(*both(up, down, second))
    up, down = ring(*both(up, down, first))

    high, low, ahead, back = dct_parts()
    ones = jnp.asarray(np.kron(np.eye(TILE // BLOCK), np.ones((BLOCK, BLOCK))), jnp.bfloat16)
    wide = jnp.repeat(offsets[0], BLOCK, axis=1)
    kept = panel // STRIDE
    flops = 6 * 2 * 2 * panel * TILE * TILE
    tables = (high, low, ahead, ones)
    product, momentum_near, wide_near, *tables_near = call(
        base_kernel,
        [shaped(panel, width, dtype=jnp.float32), shaped(panel, width), shaped(*wide.shape, dtype=jnp.int32)]
        + [shaped(*table.shape) for table in tables],
        work,
    )(weights, first, momentum[0], wide, *tables)
    summed, decoded, sent = pl.pallas_call(
        forward_kernel,
        out_shape=(shaped(panel, width), shaped(kept, width, dtype=jnp.float32), shaped(groups, kept, width)),
        in_specs=[whole, apart, apart] + [whole] * 6,
        out_specs=(apart, whole, whole),
        scratch_shapes=(
            pltpu.VMEM((kept, width), jnp.float32),
            pltpu.VMEM((panel, width), jnp.bfloat16),
            pltpu.VMEM((2, panel, width), jnp.bfloat16),
            pltpu.SemaphoreType.DMA((3, panel // TILE)),
        ),
        compiler_params=pltpu.CompilerParams(vmem_limit_bytes=GRANT),
        cost_estimate=pl.CostEstimate(flops=flops, bytes_accessed=2 << 20, transcendentals=0),
    )(product, up, down, momentum_near, wide_near, *tables_near)
    parts = lax.all_to_all(sent, "rep", 0, 0, tiled=True)
    residual = call(residual_kernel, shaped(panel, width), flops)(momentum[0], summed, decoded, wide, high, low, back)
    update = call(update_kernel, shaped(panel, width), flops)(parts, wide, high, low, back)
    return residual[None], update[None]


def solution(mesh):
    return jax.shard_map(
        step,
        mesh=mesh,
        in_specs=(
            P(None, "rep", "shard", None),
            P(None, "rep", "shard", None),
            P(None, "rep", "shard"),
            P(None, None, "shard"),
            P("rep", None, "shard"),
        ),
        out_specs=(P("rep", None, "shard"), P(None, None, "shard")),
        check_vma=False,
    )
```

```python
import functools
import math

import jax
import jax.numpy as jnp
import numpy as np
from jax import lax
from jax.experimental import pallas as pl
from jax.experimental.pallas import tpu as pltpu
from jax.sharding import PartitionSpec as P


BLOCK = 64
STRIDE = 16
DOCS = 16
LINES = 8
BETA = 0.9
CLIP = 2.0
EPS = 1e-06


TILE = 256
GRANT = 16 << 20
FULL = 60 << 20


def dct_parts():
    freq = np.arange(BLOCK, dtype=np.float64)[:, None]
    place = np.arange(BLOCK, dtype=np.float64)[None, :]
    table = np.cos(math.pi * (2.0 * place + 1.0) * freq / (2.0 * BLOCK)) * math.sqrt(2.0 / BLOCK)
    table[0] /= math.sqrt(2.0)
    whole = np.kron(np.eye(TILE // BLOCK), table)
    high = whole.astype(jnp.bfloat16)
    low = (whole - high.astype(np.float64)).astype(jnp.bfloat16)
    some = slice(0, BLOCK)
    ahead = np.concatenate([high[some, some], high[some, some], low[some, some]], axis=1)
    back = np.concatenate([high[some, some].T, high[some, some].T, low[some, some].T], axis=1)
    return tuple(jnp.asarray(part) for part in (high, low, ahead, back))


def dot(a, b, dims):
    return lax.dot_general(a, b, (dims, ((), ())), preferred_element_type=jnp.float32)


def split(x):
    high = x.astype(jnp.bfloat16)
    return high, (x - high.astype(jnp.float32)).astype(jnp.bfloat16)


def left(table, x):
    high, low = split(x)
    dims = ((1,), (0,))
    out = []
    for i in range(x.shape[0] // BLOCK):
        here = slice(i * BLOCK, (i + 1) * BLOCK)
        out.append(dot(table, jnp.concatenate([high[here], low[here], high[here]], axis=0), dims))
    return jnp.concatenate(out, axis=0)


def right(x, table, dim):
    (th, tl), (xh, xl) = table, split(x)
    dims = ((1,), (dim,))
    return dot(xh, th, dims) + (dot(xl, th, dims) + dot(xh, tl, dims))


def selected(offsets):
    count, width = offsets.shape
    shape = (count, BLOCK, width)
    both = lax.broadcasted_iota(jnp.int32, shape, 1) + lax.broadcasted_iota(jnp.int32, shape, 2)
    return ((both & (STRIDE - 1)) == offsets[:, None, :]).reshape(count * BLOCK, width)


def gathered(exchanged, start, size):
    deep = exchanged.shape[0]
    z = lax.axis_index("shard") % deep
    return jnp.concatenate([exchanged[(z - k + deep) % deep, :, start : start + size] for k in range(deep)], axis=0)


def fetch(rows, deep, width, moves, sem):
    me = lax.axis_index("shard")
    line = me // deep
    copies = []
    for i, (owner, z, target) in enumerate(moves):
        block = (line + owner + LINES) % LINES * deep + z
        column = pl.multiple_of(block * width, width)
        copies.append(pltpu.make_async_copy(rows.at[:, pl.ds(column, width)], target, sem.at[i]))
    for copy in copies:
        copy.start()
    return copies


def early_kernel(rows, grads, out, sem, given):
    deep = out.shape[0]
    panel = grads.shape[1]
    width = out.shape[2] - panel
    moves = [(4, z, out.at[z, :, pl.ds(panel, width)]) for z in range(deep)]
    copies = fetch(rows, deep, width, moves, sem)
    for z in range(deep):
        copies.append(pltpu.make_async_copy(grads, out.at[z, :, pl.ds(0, panel)], given.at[z]))
        copies[-1].start()
    for copy in copies:
        copy.wait()


def late_kernel(rows, *rest):
    third, (second, first, sem) = rest[:-3], rest[-3:]
    deep = len(third)
    width = second.shape[2] // 2
    me = lax.axis_index("shard") % deep
    moves = []
    for k in range(deep):
        for j, owner in enumerate((3, -3)):
            moves.append((owner, (me + k) % deep, third[k].at[:, pl.ds(j * width, width)]))
    for target, owners in ((second, (2, -2)), (first, (1, -1, 0))):
        for z in range(deep):
            for j, owner in enumerate(owners):
                moves.append((owner, z, target.at[z, :, pl.ds(j * width, width)]))
    for copy in fetch(rows, deep, width, moves, sem):
        copy.wait()


def scale_kernel(exchanged, *rest):
    notes, out = rest[:-1], rest[-1]
    deep, tokens = exchanged.shape[0], exchanged.shape[1]
    panel = out.shape[0]
    z = lax.axis_index("shard") % deep
    marks = [note[...].astype(jnp.float32) for note in notes]
    heads = marks[0][DOCS:]
    for mark in marks[1:]:
        heads = heads + mark[DOCS:]
    share = 1.0 / jnp.maximum(jnp.sum(heads, axis=1, keepdims=True), 1.0)
    for k in range(deep):
        weight = jnp.sum(marks[k][:DOCS] * share, axis=0, keepdims=True)
        block = exchanged[(z - k + deep) % deep, :, :panel].astype(jnp.float32)
        out[:, k * tokens : (k + 1) * tokens] = (block.T * weight).astype(jnp.bfloat16)


def far_kernel(weights, exchanged, up, down):
    half = up.shape[0]
    columns = gathered(exchanged, exchanged.shape[2] - up.shape[1], up.shape[1])
    dims = ((1,), (0,))
    up[...] = dot(weights[:half], columns, dims).astype(jnp.bfloat16)
    down[...] = dot(weights[half:], columns, dims).astype(jnp.bfloat16)


def far_near_kernel(start, top, weights, received, *rest):
    parts, out = rest[:-1], rest[-1]
    width = out.shape[1]
    columns = jnp.concatenate([part[:, start : start + width] for part in parts], axis=0)
    total = dot(weights[...], columns, ((1,), (0,)))
    rows = received.shape[0]
    here, other = (slice(0, rows), slice(rows, None)) if top else (slice(rows, None), slice(0, rows))
    out[here] = (total[here] + received[...].astype(jnp.float32)).astype(jnp.bfloat16)
    out[other] = total[other].astype(jnp.bfloat16)


def near_kernel(start, weights, received, exchanged, out):
    width = out.shape[1]
    total = dot(weights[...], gathered(exchanged, start, width), ((1,), (0,)))
    out[...] = (total + received[...].astype(jnp.float32)).astype(jnp.bfloat16)


def base_kernel(weights, exchanged, momentum, offsets, *rest):
    tables, (product, kept, offsets_out, *tables_out) = rest[: len(rest) // 2 - 1], rest[len(rest) // 2 - 1 :]
    product[...] = dot(weights[...], gathered(exchanged, 2 * product.shape[1], product.shape[1]), ((1,), (0,)))
    kept[...] = momentum[...]
    offsets_out[...] = offsets[...]
    for table, out in zip(tables, tables_out):
        out[...] = table[...]


def forward_kernel(
    product, up, down, momentum, offsets, high, low, ahead, ones, summed, decoded, sent, packed, held, parts, sem
):
    table = (high[...], low[...])
    per = TILE // BLOCK
    rows = TILE // STRIDE
    fetches = []
    for i in range(product.shape[0] // TILE):
        there = pl.ds(i * TILE, TILE)
        pair = [pltpu.make_async_copy(x.at[there], parts.at[j, there], sem.at[1 + j, i]) for j, x in enumerate((up, down))]
        fetches.append(pair)
        for copy in pair:
            copy.start()
    copies = []
    for i in range(product.shape[0] // TILE):
        here = slice(i * TILE, (i + 1) * TILE)
        for copy in fetches[i]:
            copy.wait()
        total = product[here] + parts[0, here].astype(jnp.float32) + parts[1, here].astype(jnp.float32)
        gradient = total.astype(jnp.bfloat16)
        held[here] = gradient
        copies.append(pltpu.make_async_copy(held.at[pl.ds(i * TILE, TILE)], summed.at[pl.ds(i * TILE, TILE)], sem.at[0, i]))
        copies[-1].start()
        value = BETA * momentum[here].astype(jnp.float32) + gradient.astype(jnp.float32)
        spectrum = right(left(ahead[...], value), table, 1)
        kept = jnp.where(selected(offsets[i * per : (i + 1) * per]), spectrum, 0.0)
        packed[i * rows : (i + 1) * rows] = jnp.sum(kept.reshape(rows, STRIDE, TILE), axis=1)
    values = packed[...]
    group = BLOCK // STRIDE
    squares = jnp.sum((values * values).reshape(-1, group, TILE), axis=1)
    first = squares.astype(jnp.bfloat16)
    rest = squares - first.astype(jnp.float32)
    second, third = split(rest)
    dims = ((1,), (0,))
    total = dot(first, ones[...], dims) + (dot(second, ones[...], dims) + dot(third, ones[...], dims))
    mean = total * (1.0 / (BLOCK * group))
    scale = (CLIP * jnp.sqrt(mean + EPS)).astype(jnp.bfloat16).astype(jnp.float32)
    spread = jnp.broadcast_to(scale[:, None, :], (scale.shape[0], group, TILE)).reshape(values.shape)
    quantized = jnp.clip(values / spread, -1.0, 1.0).astype(jnp.bfloat16)
    result = quantized.astype(jnp.float32) * spread
    decoded[...] = result
    rounded = result.astype(jnp.bfloat16)
    for k in range(sent.shape[0]):
        sent[k] = rounded
    for copy in copies:
        copy.wait()


def spread_tile(values, offsets):
    rows, width = values.shape
    wide = jnp.broadcast_to(values[:, None, :], (rows, STRIDE, width)).reshape(rows * STRIDE, width)
    return jnp.where(selected(offsets), wide, 0.0)


def inverse_tile(values, offsets, table, back):
    return right(left(back, spread_tile(values, offsets)), table, 0)


def residual_kernel(momentum, summed, decoded, offsets, high, low, back_table, out):
    table = (high[...], low[...])
    per = TILE // BLOCK
    rows = TILE // STRIDE
    for i in range(out.shape[0] // TILE):
        here = slice(i * TILE, (i + 1) * TILE)
        value = BETA * momentum[here].astype(jnp.float32) + summed[here].astype(jnp.float32)
        back = inverse_tile(decoded[i * rows : (i + 1) * rows], offsets[i * per : (i + 1) * per], table, back_table[...])
        out[here] = (value - back).astype(jnp.bfloat16)


def update_kernel(parts, offsets, high, low, back_table, out):
    table = (high[...], low[...])
    per = TILE // BLOCK
    rows = TILE // STRIDE
    count = parts.shape[0]
    for i in range(out.shape[0] // TILE):
        here = slice(i * rows, (i + 1) * rows)
        total = parts[0, here].astype(jnp.float32)
        for k in range(1, count):
            total += parts[k, here].astype(jnp.float32)
        back = inverse_tile(total * (1.0 / count), offsets[i * per : (i + 1) * per], table, back_table[...])
        out[i * TILE : (i + 1) * TILE] = back.astype(jnp.bfloat16)


def call(kernel, out_shape, flops, scratch=(), in_specs=None, grant=GRANT):
    extra = {} if in_specs is None else {"in_specs": in_specs}
    return pl.pallas_call(
        kernel,
        out_shape=out_shape,
        scratch_shapes=scratch,
        compiler_params=pltpu.CompilerParams(vmem_limit_bytes=grant),
        cost_estimate=pl.CostEstimate(flops=flops, bytes_accessed=2 << 20, transcendentals=0),
        **extra,
    )


def shaped(*shape, dtype=jnp.bfloat16):
    return jax.ShapeDtypeStruct(shape, dtype)


def step(features, out_grads, doc_ids, offsets, momentum):
    shards = lax.axis_size("shard")
    deep = shards // LINES
    groups = lax.axis_size("rep")

    def along_line(x, k):
        pairs = [(y * deep + z, y * deep + (z + k) % deep) for y in range(LINES) for z in range(deep)]
        return lax.ppermute(x, "shard", pairs)

    def across(x, k):
        pairs = [(y * deep + z, (y + k) % LINES * deep + z) for y in range(LINES) for z in range(deep)]
        return lax.ppermute(x, "shard", pairs)

    def exchange(x):
        lines = [[y * deep + z for z in range(deep)] for y in range(LINES)]
        return lax.all_to_all(x, "shard", 0, 0, axis_index_groups=lines, tiled=True)

    rows = features[0, 0]
    grads = out_grads[0, 0]
    tokens, panel = grads.shape
    width = rows.shape[1] // shards
    whole = pl.BlockSpec(memory_space=pltpu.VMEM)
    apart = pl.BlockSpec(memory_space=pltpu.HBM)
    work = 2 * panel * deep * tokens * width

    early = call(
        early_kernel,
        shaped(deep, tokens, panel + width),
        work,
        (pltpu.SemaphoreType.DMA((deep,)), pltpu.SemaphoreType.DMA((deep,))),
        [apart, apart],
        FULL,
    )(rows, grads)
    early = exchange(early)

    documents = lax.broadcasted_iota(jnp.int32, (DOCS, tokens), 0)
    onehot = (doc_ids[0] == documents).astype(jnp.float32)
    counts = jnp.broadcast_to(jnp.sum(onehot, axis=1, keepdims=True), (DOCS, tokens))
    before = across(counts, 1)
    after = across(counts, -1)
    lane = lax.broadcasted_iota(jnp.int32, (DOCS, tokens), 1)
    heads = jnp.where(lane == 0, counts, jnp.where(lane == 1, before, jnp.where(lane == 2, after, 0.0)))
    extra = jnp.concatenate([onehot, heads], axis=0).astype(jnp.bfloat16)

    notes = [extra]
    for k in (2, 1, 3):
        notes.append(along_line(extra, k))
    notes = [notes[0], notes[2], notes[1], notes[3]]

    *third, second, first = call(
        late_kernel,
        [shaped(tokens, 2 * width)] * deep + [shaped(deep, tokens, 2 * width), shaped(deep, tokens, 3 * width)],
        work,
        (pltpu.SemaphoreType.DMA((7 * deep,)),),
        [apart],
        FULL,
    )(rows)
    for k in (2, 1, 3):
        third[k] = along_line(third[k], k)
    second = exchange(second)
    first = exchange(first)

    weights = call(scale_kernel, shaped(panel, deep * tokens), work)(early, *notes)
    half = panel // 2
    up, down = call(far_kernel, [shaped(half, width)] * 2, work)(weights, early)

    def ring(up, down):
        up = across(up, 1)
        down = across(down, -1)
        return up, down

    def near(kernel, received, *given):
        return call(kernel, shaped(panel, width), work)(weights, received, *given)

    def both(up, down, exchanged):
        first_half, second_half = functools.partial(near_kernel, 0), functools.partial(near_kernel, width)
        return near(first_half, up, exchanged), near(second_half, down, exchanged)

    up, down = ring(up, down)
    up = near(functools.partial(far_near_kernel, 0, True), up, *third)
    down = near(functools.partial(far_near_kernel, width, False), down, *third)
    up, down = ring(up, down)
    up, down = ring(*both(up, down, second))
    up, down = ring(*both(up, down, first))

    high, low, ahead, back = dct_parts()
    ones = jnp.asarray(np.kron(np.eye(TILE // BLOCK), np.ones((BLOCK, BLOCK))), jnp.bfloat16)
    wide = jnp.repeat(offsets[0], BLOCK, axis=1)
    kept = panel // STRIDE
    flops = 6 * 2 * 2 * panel * TILE * TILE
    tables = (high, low, ahead, ones)
    product, momentum_near, wide_near, *tables_near = call(
        base_kernel,
        [shaped(panel, width, dtype=jnp.float32), shaped(panel, width), shaped(*wide.shape, dtype=jnp.int32)]
        + [shaped(*table.shape) for table in tables],
        work,
    )(weights, first, momentum[0], wide, *tables)
    summed, decoded, sent = pl.pallas_call(
        forward_kernel,
        out_shape=(shaped(panel, width), shaped(kept, width, dtype=jnp.float32), shaped(groups, kept, width)),
        in_specs=[whole, apart, apart] + [whole] * 6,
        out_specs=(apart, whole, whole),
        scratch_shapes=(
            pltpu.VMEM((kept, width), jnp.float32),
            pltpu.VMEM((panel, width), jnp.bfloat16),
            pltpu.VMEM((2, panel, width), jnp.bfloat16),
            pltpu.SemaphoreType.DMA((3, panel // TILE)),
        ),
        compiler_params=pltpu.CompilerParams(vmem_limit_bytes=GRANT),
        cost_estimate=pl.CostEstimate(flops=flops, bytes_accessed=2 << 20, transcendentals=0),
    )(product, up, down, momentum_near, wide_near, *tables_near)
    parts = lax.all_to_all(sent, "rep", 0, 0, tiled=True)
    residual = call(residual_kernel, shaped(panel, width), flops)(momentum[0], summed, decoded, wide, high, low, back)
    update = call(update_kernel, shaped(panel, width), flops)(parts, wide, high, low, back)
    return residual[None], update[None]


def solution(mesh):
    return jax.shard_map(
        step,
        mesh=mesh,
        in_specs=(
            P(None, "rep", "shard", None),
            P(None, "rep", "shard", None),
            P(None, "rep", "shard"),
            P(None, None, "shard"),
            P("rep", None, "shard"),
        ),
        out_specs=(P("rep", None, "shard"), P(None, None, "shard")),
        check_vma=False,
    )
```

```python
import functools
import math

import jax
import jax.numpy as jnp
import numpy as np
from jax import lax
from jax.experimental import pallas as pl
from jax.experimental.pallas import tpu as pltpu
from jax.sharding import PartitionSpec as P


BLOCK = 64
STRIDE = 16
DOCS = 16
LINES = 8
BETA = 0.9
CLIP = 2.0
EPS = 1e-06


TILE = 256
GRANT = 16 << 20
FULL = 60 << 20


def dct_parts():
    freq = np.arange(BLOCK, dtype=np.float64)[:, None]
    place = np.arange(BLOCK, dtype=np.float64)[None, :]
    table = np.cos(math.pi * (2.0 * place + 1.0) * freq / (2.0 * BLOCK)) * math.sqrt(2.0 / BLOCK)
    table[0] /= math.sqrt(2.0)
    whole = np.kron(np.eye(TILE // BLOCK), table)
    high = whole.astype(jnp.bfloat16)
    low = (whole - high.astype(np.float64)).astype(jnp.bfloat16)
    some = slice(0, BLOCK)
    ahead = np.concatenate([high[some, some], high[some, some], low[some, some]], axis=1)
    back = np.concatenate([high[some, some].T, high[some, some].T, low[some, some].T], axis=1)
    return tuple(jnp.asarray(part) for part in (high, low, ahead, back))


def dot(a, b, dims):
    return lax.dot_general(a, b, (dims, ((), ())), preferred_element_type=jnp.float32)


def split(x):
    high = x.astype(jnp.bfloat16)
    return high, (x - high.astype(jnp.float32)).astype(jnp.bfloat16)


def left(table, x):
    high, low = split(x)
    dims = ((1,), (0,))
    out = []
    for i in range(x.shape[0] // BLOCK):
        here = slice(i * BLOCK, (i + 1) * BLOCK)
        out.append(dot(table, jnp.concatenate([high[here], low[here], high[here]], axis=0), dims))
    return jnp.concatenate(out, axis=0)


def right(x, table, dim):
    (th, tl), (xh, xl) = table, split(x)
    dims = ((1,), (dim,))
    return dot(xh, th, dims) + (dot(xl, th, dims) + dot(xh, tl, dims))


def selected(offsets):
    count, width = offsets.shape
    shape = (count, BLOCK, width)
    both = lax.broadcasted_iota(jnp.int32, shape, 1) + lax.broadcasted_iota(jnp.int32, shape, 2)
    return ((both & (STRIDE - 1)) == offsets[:, None, :]).reshape(count * BLOCK, width)


def gathered(exchanged, start, size):
    deep = exchanged.shape[0]
    z = lax.axis_index("shard") % deep
    return jnp.concatenate([exchanged[(z - k + deep) % deep, :, start : start + size] for k in range(deep)], axis=0)


def fetch(rows, deep, width, moves, sem):
    me = lax.axis_index("shard")
    line = me // deep
    copies = []
    for i, (owner, z, target) in enumerate(moves):
        block = (line + owner + LINES) % LINES * deep + z
        column = pl.multiple_of(block * width, width)
        copies.append(pltpu.make_async_copy(rows.at[:, pl.ds(column, width)], target, sem.at[i]))
    for copy in copies:
        copy.start()
    return copies


def gather_kernel(rows, grads, *rest):
    *outs, sem, given = rest
    deep = outs[0].shape[0]
    early, second, first = outs[:3]
    third, own = outs[3 : 3 + deep], outs[3 + deep :]
    panel = grads.shape[1]
    width = early.shape[2] - panel
    me = lax.axis_index("shard") % deep
    moves = [(4, z, early.at[z, :, pl.ds(panel, width)]) for z in range(deep)]
    for k in range(deep):
        z = (me + k) % deep
        for j, owner in enumerate((3, -3)):
            moves.append((owner, z, third[k].at[:, pl.ds(j * width, width)]))
        moves.append((0, z, own[k]))
    for target, owners in ((second, (2, -2)), (first, (1, -1))):
        for z in range(deep):
            for j, owner in enumerate(owners):
                moves.append((owner, z, target.at[z, :, pl.ds(j * width, width)]))
    copies = fetch(rows, deep, width, moves, sem)
    for z in range(deep):
        copies.append(pltpu.make_async_copy(grads, early.at[z, :, pl.ds(0, panel)], given.at[z]))
        copies[-1].start()
    for copy in copies:
        copy.wait()


def scale_kernel(exchanged, *rest):
    notes, out = rest[:-1], rest[-1]
    deep, tokens = exchanged.shape[0], exchanged.shape[1]
    panel = out.shape[0]
    z = lax.axis_index("shard") % deep
    marks = [note[...].astype(jnp.float32) for note in notes]
    heads = marks[0][DOCS:]
    for mark in marks[1:]:
        heads = heads + mark[DOCS:]
    share = 1.0 / jnp.maximum(jnp.sum(heads, axis=1, keepdims=True), 1.0)
    for k in range(deep):
        weight = jnp.sum(marks[k][:DOCS] * share, axis=0, keepdims=True)
        block = exchanged[(z - k + deep) % deep, :, :panel].astype(jnp.float32)
        out[:, k * tokens : (k + 1) * tokens] = (block.T * weight).astype(jnp.bfloat16)


def far_kernel(weights, exchanged, up, down):
    half = up.shape[0]
    columns = gathered(exchanged, exchanged.shape[2] - up.shape[1], up.shape[1])
    dims = ((1,), (0,))
    up[...] = dot(weights[:half], columns, dims).astype(jnp.bfloat16)
    down[...] = dot(weights[half:], columns, dims).astype(jnp.bfloat16)


def far_near_kernel(start, top, weights, received, *rest):
    parts, out = rest[:-1], rest[-1]
    width = out.shape[1]
    columns = jnp.concatenate([part[:, start : start + width] for part in parts], axis=0)
    total = dot(weights[...], columns, ((1,), (0,)))
    rows = received.shape[0]
    here, other = (slice(0, rows), slice(rows, None)) if top else (slice(rows, None), slice(0, rows))
    out[here] = (total[here] + received[...].astype(jnp.float32)).astype(jnp.bfloat16)
    out[other] = total[other].astype(jnp.bfloat16)


def near_kernel(start, weights, received, exchanged, out):
    width = out.shape[1]
    total = dot(weights[...], gathered(exchanged, start, width), ((1,), (0,)))
    out[...] = (total + received[...].astype(jnp.float32)).astype(jnp.bfloat16)


def base_kernel(count, *rest):
    parts, (weights, momentum, offsets, *rest) = rest[:count], rest[count:]
    half = len(rest) // 2 - 1
    tables, (product, kept, offsets_out, *tables_out) = rest[:half], rest[half:]
    columns = jnp.concatenate([part[...] for part in parts], axis=0)
    product[...] = dot(weights[...], columns, ((1,), (0,)))
    kept[...] = momentum[...]
    offsets_out[...] = offsets[...]
    for table, out in zip(tables, tables_out):
        out[...] = table[...]


def forward_kernel(
    product, up, down, momentum, offsets, high, low, ahead, ones, summed, decoded, sent, packed, held, parts, sem
):
    table = (high[...], low[...])
    per = TILE // BLOCK
    rows = TILE // STRIDE
    fetches = []
    for i in range(product.shape[0] // TILE):
        there = pl.ds(i * TILE, TILE)
        pair = [pltpu.make_async_copy(x.at[there], parts.at[j, there], sem.at[1 + j, i]) for j, x in enumerate((up, down))]
        fetches.append(pair)
        for copy in pair:
            copy.start()
    copies = []
    for i in range(product.shape[0] // TILE):
        here = slice(i * TILE, (i + 1) * TILE)
        for copy in fetches[i]:
            copy.wait()
        total = product[here] + parts[0, here].astype(jnp.float32) + parts[1, here].astype(jnp.float32)
        gradient = total.astype(jnp.bfloat16)
        held[here] = gradient
        copies.append(pltpu.make_async_copy(held.at[pl.ds(i * TILE, TILE)], summed.at[pl.ds(i * TILE, TILE)], sem.at[0, i]))
        copies[-1].start()
        value = BETA * momentum[here].astype(jnp.float32) + gradient.astype(jnp.float32)
        spectrum = right(left(ahead[...], value), table, 1)
        kept = jnp.where(selected(offsets[i * per : (i + 1) * per]), spectrum, 0.0)
        packed[i * rows : (i + 1) * rows] = jnp.sum(kept.reshape(rows, STRIDE, TILE), axis=1)
    values = packed[...]
    group = BLOCK // STRIDE
    squares = jnp.sum((values * values).reshape(-1, group, TILE), axis=1)
    first = squares.astype(jnp.bfloat16)
    rest = squares - first.astype(jnp.float32)
    second, third = split(rest)
    dims = ((1,), (0,))
    total = dot(first, ones[...], dims) + (dot(second, ones[...], dims) + dot(third, ones[...], dims))
    mean = total * (1.0 / (BLOCK * group))
    scale = (CLIP * jnp.sqrt(mean + EPS)).astype(jnp.bfloat16).astype(jnp.float32)
    spread = jnp.broadcast_to(scale[:, None, :], (scale.shape[0], group, TILE)).reshape(values.shape)
    quantized = jnp.clip(values / spread, -1.0, 1.0).astype(jnp.bfloat16)
    result = quantized.astype(jnp.float32) * spread
    decoded[...] = result
    rounded = result.astype(jnp.bfloat16)
    for k in range(sent.shape[0]):
        sent[k] = rounded
    for copy in copies:
        copy.wait()


def spread_tile(values, offsets):
    rows, width = values.shape
    wide = jnp.broadcast_to(values[:, None, :], (rows, STRIDE, width)).reshape(rows * STRIDE, width)
    return jnp.where(selected(offsets), wide, 0.0)


def inverse_tile(values, offsets, table, back):
    return right(left(back, spread_tile(values, offsets)), table, 0)


def residual_kernel(momentum, summed, decoded, offsets, high, low, back_table, out):
    table = (high[...], low[...])
    per = TILE // BLOCK
    rows = TILE // STRIDE
    for i in range(out.shape[0] // TILE):
        here = slice(i * TILE, (i + 1) * TILE)
        value = BETA * momentum[here].astype(jnp.float32) + summed[here].astype(jnp.float32)
        back = inverse_tile(decoded[i * rows : (i + 1) * rows], offsets[i * per : (i + 1) * per], table, back_table[...])
        out[here] = (value - back).astype(jnp.bfloat16)


def update_kernel(parts, offsets, high, low, back_table, out):
    table = (high[...], low[...])
    per = TILE // BLOCK
    rows = TILE // STRIDE
    count = parts.shape[0]
    for i in range(out.shape[0] // TILE):
        here = slice(i * rows, (i + 1) * rows)
        total = parts[0, here].astype(jnp.float32)
        for k in range(1, count):
            total += parts[k, here].astype(jnp.float32)
        back = inverse_tile(total * (1.0 / count), offsets[i * per : (i + 1) * per], table, back_table[...])
        out[i * TILE : (i + 1) * TILE] = back.astype(jnp.bfloat16)


def call(kernel, out_shape, flops, scratch=(), in_specs=None, grant=GRANT):
    extra = {} if in_specs is None else {"in_specs": in_specs}
    return pl.pallas_call(
        kernel,
        out_shape=out_shape,
        scratch_shapes=scratch,
        compiler_params=pltpu.CompilerParams(vmem_limit_bytes=grant),
        cost_estimate=pl.CostEstimate(flops=flops, bytes_accessed=2 << 20, transcendentals=0),
        **extra,
    )


def shaped(*shape, dtype=jnp.bfloat16):
    return jax.ShapeDtypeStruct(shape, dtype)


def step(features, out_grads, doc_ids, offsets, momentum):
    shards = lax.axis_size("shard")
    deep = shards // LINES
    groups = lax.axis_size("rep")

    def along_line(x, k):
        pairs = [(y * deep + z, y * deep + (z + k) % deep) for y in range(LINES) for z in range(deep)]
        return lax.ppermute(x, "shard", pairs)

    def across(x, k):
        pairs = [(y * deep + z, (y + k) % LINES * deep + z) for y in range(LINES) for z in range(deep)]
        return lax.ppermute(x, "shard", pairs)

    def exchange(x):
        lines = [[y * deep + z for z in range(deep)] for y in range(LINES)]
        return lax.all_to_all(x, "shard", 0, 0, axis_index_groups=lines, tiled=True)

    rows = features[0, 0]
    grads = out_grads[0, 0]
    tokens, panel = grads.shape
    width = rows.shape[1] // shards
    whole = pl.BlockSpec(memory_space=pltpu.VMEM)
    apart = pl.BlockSpec(memory_space=pltpu.HBM)
    work = 2 * panel * deep * tokens * width

    early, second, first, *others = call(
        gather_kernel,
        [shaped(deep, tokens, panel + width)]
        + [shaped(deep, tokens, 2 * width)] * 2
        + [shaped(tokens, 2 * width)] * deep
        + [shaped(tokens, width)] * deep,
        work,
        (pltpu.SemaphoreType.DMA((8 * deep,)), pltpu.SemaphoreType.DMA((deep,))),
        [apart, apart],
        FULL,
    )(rows, grads)
    third, own = others[:deep], others[deep:]
    early = exchange(early)

    documents = lax.broadcasted_iota(jnp.int32, (DOCS, tokens), 0)
    onehot = (doc_ids[0] == documents).astype(jnp.float32)
    counts = jnp.broadcast_to(jnp.sum(onehot, axis=1, keepdims=True), (DOCS, tokens))
    before = across(counts, 1)
    after = across(counts, -1)
    lane = lax.broadcasted_iota(jnp.int32, (DOCS, tokens), 1)
    heads = jnp.where(lane == 0, counts, jnp.where(lane == 1, before, jnp.where(lane == 2, after, 0.0)))
    extra = jnp.concatenate([onehot, heads], axis=0).astype(jnp.bfloat16)

    notes = [extra]
    for k in (2, 1, 3):
        notes.append(along_line(extra, k))
    notes = [notes[0], notes[2], notes[1], notes[3]]

    for k in (2, 1, 3):
        third[k] = along_line(third[k], k)
    for k in (2, 1, 3):
        own[k] = along_line(own[k], k)
    second = exchange(second)
    first = exchange(first)

    weights = call(scale_kernel, shaped(panel, deep * tokens), work)(early, *notes)
    half = panel // 2
    up, down = call(far_kernel, [shaped(half, width)] * 2, work)(weights, early)

    def ring(up, down):
        up = across(up, 1)
        down = across(down, -1)
        return up, down

    def near(kernel, received, *given):
        return call(kernel, shaped(panel, width), work)(weights, received, *given)

    def both(up, down, exchanged):
        first_half, second_half = functools.partial(near_kernel, 0), functools.partial(near_kernel, width)
        return near(first_half, up, exchanged), near(second_half, down, exchanged)

    up, down = ring(up, down)
    up = near(functools.partial(far_near_kernel, 0, True), up, *third)
    down = near(functools.partial(far_near_kernel, width, False), down, *third)
    up, down = ring(up, down)
    up, down = ring(*both(up, down, second))
    up, down = ring(*both(up, down, first))

    high, low, ahead, back = dct_parts()
    ones = jnp.asarray(np.kron(np.eye(TILE // BLOCK), np.ones((BLOCK, BLOCK))), jnp.bfloat16)
    wide = jnp.repeat(offsets[0], BLOCK, axis=1)
    kept = panel // STRIDE
    flops = 6 * 2 * 2 * panel * TILE * TILE
    tables = (high, low, ahead, ones)
    product, momentum_near, wide_near, *tables_near = call(
        functools.partial(base_kernel, deep),
        [shaped(panel, width, dtype=jnp.float32), shaped(panel, width), shaped(*wide.shape, dtype=jnp.int32)]
        + [shaped(*table.shape) for table in tables],
        work,
    )(*own, weights, momentum[0], wide, *tables)
    summed, decoded, sent = pl.pallas_call(
        forward_kernel,
        out_shape=(shaped(panel, width), shaped(kept, width, dtype=jnp.float32), shaped(groups, kept, width)),
        in_specs=[whole, apart, apart] + [whole] * 6,
        out_specs=(apart, whole, whole),
        scratch_shapes=(
            pltpu.VMEM((kept, width), jnp.float32),
            pltpu.VMEM((panel, width), jnp.bfloat16),
            pltpu.VMEM((2, panel, width), jnp.bfloat16),
            pltpu.SemaphoreType.DMA((3, panel // TILE)),
        ),
        compiler_params=pltpu.CompilerParams(vmem_limit_bytes=GRANT),
        cost_estimate=pl.CostEstimate(flops=flops, bytes_accessed=2 << 20, transcendentals=0),
    )(product, up, down, momentum_near, wide_near, *tables_near)
    parts = lax.all_to_all(sent, "rep", 0, 0, tiled=True)
    residual = call(residual_kernel, shaped(panel, width), flops)(momentum[0], summed, decoded, wide, high, low, back)
    update = call(update_kernel, shaped(panel, width), flops)(parts, wide, high, low, back)
    return residual[None], update[None]


def solution(mesh):
    return jax.shard_map(
        step,
        mesh=mesh,
        in_specs=(
            P(None, "rep", "shard", None),
            P(None, "rep", "shard", None),
            P(None, "rep", "shard"),
            P(None, None, "shard"),
            P("rep", None, "shard"),
        ),
        out_specs=(P("rep", None, "shard"), P(None, None, "shard")),
        check_vma=False,
    )
```

```python
import functools
import math

import jax
import jax.numpy as jnp
import numpy as np
from jax import lax
from jax.experimental import pallas as pl
from jax.experimental.pallas import tpu as pltpu
from jax.sharding import PartitionSpec as P


BLOCK = 64
STRIDE = 16
DOCS = 16
LINES = 8
BETA = 0.9
CLIP = 2.0
EPS = 1e-06


TILE = 256
GRANT = 16 << 20
FULL = 60 << 20


def dct_parts():
    freq = np.arange(BLOCK, dtype=np.float64)[:, None]
    place = np.arange(BLOCK, dtype=np.float64)[None, :]
    table = np.cos(math.pi * (2.0 * place + 1.0) * freq / (2.0 * BLOCK)) * math.sqrt(2.0 / BLOCK)
    table[0] /= math.sqrt(2.0)
    whole = np.kron(np.eye(TILE // BLOCK), table)
    high = whole.astype(jnp.bfloat16)
    low = (whole - high.astype(np.float64)).astype(jnp.bfloat16)
    some = slice(0, BLOCK)
    ahead = np.concatenate([high[some, some], high[some, some], low[some, some]], axis=1)
    back = np.concatenate([high[some, some].T, high[some, some].T, low[some, some].T], axis=1)
    return tuple(jnp.asarray(part) for part in (high, low, ahead, back))


def dot(a, b, dims):
    return lax.dot_general(a, b, (dims, ((), ())), preferred_element_type=jnp.float32)


def split(x):
    high = x.astype(jnp.bfloat16)
    return high, (x - high.astype(jnp.float32)).astype(jnp.bfloat16)


def left(table, x):
    high, low = split(x)
    dims = ((1,), (0,))
    out = []
    for i in range(x.shape[0] // BLOCK):
        here = slice(i * BLOCK, (i + 1) * BLOCK)
        out.append(dot(table, jnp.concatenate([high[here], low[here], high[here]], axis=0), dims))
    return jnp.concatenate(out, axis=0)


def right(x, table, dim):
    (th, tl), (xh, xl) = table, split(x)
    dims = ((1,), (dim,))
    return dot(xh, th, dims) + (dot(xl, th, dims) + dot(xh, tl, dims))


def selected(offsets):
    count, width = offsets.shape
    shape = (count, BLOCK, width)
    both = lax.broadcasted_iota(jnp.int32, shape, 1) + lax.broadcasted_iota(jnp.int32, shape, 2)
    return ((both & (STRIDE - 1)) == offsets[:, None, :]).reshape(count * BLOCK, width)


def gathered(exchanged, start, size):
    deep = exchanged.shape[0]
    z = lax.axis_index("shard") % deep
    return jnp.concatenate([exchanged[(z - k + deep) % deep, :, start : start + size] for k in range(deep)], axis=0)


def fetch(rows, deep, width, moves, sem):
    me = lax.axis_index("shard")
    line = me // deep
    copies = []
    for i, (owner, z, target) in enumerate(moves):
        block = (line + owner + LINES) % LINES * deep + z
        column = pl.multiple_of(block * width, width)
        copies.append(pltpu.make_async_copy(rows.at[:, pl.ds(column, width)], target, sem.at[i]))
    for copy in copies:
        copy.start()
    return copies


def early_kernel(rows, grads, out, sem, given):
    deep = out.shape[0]
    panel = grads.shape[1]
    width = out.shape[2] - panel
    moves = [(4, z, out.at[z, :, pl.ds(panel, width)]) for z in range(deep)]
    copies = fetch(rows, deep, width, moves, sem)
    for z in range(deep):
        copies.append(pltpu.make_async_copy(grads, out.at[z, :, pl.ds(0, panel)], given.at[z]))
        copies[-1].start()
    for copy in copies:
        copy.wait()


def late_kernel(rows, third, second, first, sem):
    deep = third.shape[0]
    width = third.shape[2] // 2
    moves = []
    for target, owners in ((third, (3, -3)), (second, (2, -2)), (first, (1, -1, 0))):
        for z in range(deep):
            for j, owner in enumerate(owners):
                moves.append((owner, z, target.at[z, :, pl.ds(j * width, width)]))
    for copy in fetch(rows, deep, width, moves, sem):
        copy.wait()


def scale_kernel(exchanged, *rest):
    notes, out = rest[:-1], rest[-1]
    deep, tokens = exchanged.shape[0], exchanged.shape[1]
    panel = out.shape[0]
    z = lax.axis_index("shard") % deep
    marks = [note[...].astype(jnp.float32) for note in notes]
    heads = marks[0][DOCS:]
    for mark in marks[1:]:
        heads = heads + mark[DOCS:]
    share = 1.0 / jnp.maximum(jnp.sum(heads, axis=1, keepdims=True), 1.0)
    for k in range(deep):
        weight = jnp.sum(marks[k][:DOCS] * share, axis=0, keepdims=True)
        block = exchanged[(z - k + deep) % deep, :, :panel].astype(jnp.float32)
        out[:, k * tokens : (k + 1) * tokens] = (block.T * weight).astype(jnp.bfloat16)


def far_kernel(weights, exchanged, up, down):
    half = up.shape[0]
    columns = gathered(exchanged, exchanged.shape[2] - up.shape[1], up.shape[1])
    dims = ((1,), (0,))
    up[...] = dot(weights[:half], columns, dims).astype(jnp.bfloat16)
    down[...] = dot(weights[half:], columns, dims).astype(jnp.bfloat16)


def near_kernel(start, top, weights, received, exchanged, out):
    width = out.shape[1]
    total = dot(weights[...], gathered(exchanged, start, width), ((1,), (0,)))
    rows = received.shape[0]
    if rows == out.shape[0]:
        out[...] = (total + received[...].astype(jnp.float32)).astype(jnp.bfloat16)
    else:
        here, other = (slice(0, rows), slice(rows, None)) if top else (slice(rows, None), slice(0, rows))
        out[here] = (total[here] + received[...].astype(jnp.float32)).astype(jnp.bfloat16)
        out[other] = total[other].astype(jnp.bfloat16)


def own_kernel(weights, exchanged, product):
    width = product.shape[1]
    product[...] = dot(weights[...], gathered(exchanged, 2 * width, width), ((1,), (0,)))


def keep_kernel(*refs):
    half = len(refs) // 2
    for given, out in zip(refs[:half], refs[half:]):
        out[...] = given[...]


def forward_kernel(
    product, up, down, momentum, offsets, high, low, ahead, ones, summed, decoded, sent, packed, held, parts, sem
):
    table = (high[...], low[...])
    per = TILE // BLOCK
    rows = TILE // STRIDE
    fetches = []
    for i in range(product.shape[0] // TILE):
        there = pl.ds(i * TILE, TILE)
        pair = [pltpu.make_async_copy(x.at[there], parts.at[j, there], sem.at[1 + j, i]) for j, x in enumerate((up, down))]
        fetches.append(pair)
        for copy in pair:
            copy.start()
    copies = []
    for i in range(product.shape[0] // TILE):
        here = slice(i * TILE, (i + 1) * TILE)
        for copy in fetches[i]:
            copy.wait()
        total = product[here] + parts[0, here].astype(jnp.float32) + parts[1, here].astype(jnp.float32)
        gradient = total.astype(jnp.bfloat16)
        held[here] = gradient
        copies.append(pltpu.make_async_copy(held.at[pl.ds(i * TILE, TILE)], summed.at[pl.ds(i * TILE, TILE)], sem.at[0, i]))
        copies[-1].start()
        value = BETA * momentum[here].astype(jnp.float32) + gradient.astype(jnp.float32)
        spectrum = right(left(ahead[...], value), table, 1)
        kept = jnp.where(selected(offsets[i * per : (i + 1) * per]), spectrum, 0.0)
        packed[i * rows : (i + 1) * rows] = jnp.sum(kept.reshape(rows, STRIDE, TILE), axis=1)
    values = packed[...]
    group = BLOCK // STRIDE
    squares = jnp.sum((values * values).reshape(-1, group, TILE), axis=1)
    first = squares.astype(jnp.bfloat16)
    rest = squares - first.astype(jnp.float32)
    second, third = split(rest)
    dims = ((1,), (0,))
    total = dot(first, ones[...], dims) + (dot(second, ones[...], dims) + dot(third, ones[...], dims))
    mean = total * (1.0 / (BLOCK * group))
    scale = (CLIP * jnp.sqrt(mean + EPS)).astype(jnp.bfloat16).astype(jnp.float32)
    spread = jnp.broadcast_to(scale[:, None, :], (scale.shape[0], group, TILE)).reshape(values.shape)
    quantized = jnp.clip(values / spread, -1.0, 1.0).astype(jnp.bfloat16)
    result = quantized.astype(jnp.float32) * spread
    decoded[...] = result
    rounded = result.astype(jnp.bfloat16)
    for k in range(sent.shape[0]):
        sent[k] = rounded
    for copy in copies:
        copy.wait()


def spread_tile(values, offsets):
    rows, width = values.shape
    wide = jnp.broadcast_to(values[:, None, :], (rows, STRIDE, width)).reshape(rows * STRIDE, width)
    return jnp.where(selected(offsets), wide, 0.0)


def inverse_tile(values, offsets, table, back):
    return right(left(back, spread_tile(values, offsets)), table, 0)


def residual_kernel(momentum, summed, decoded, offsets, high, low, back_table, out):
    table = (high[...], low[...])
    per = TILE // BLOCK
    rows = TILE // STRIDE
    for i in range(out.shape[0] // TILE):
        here = slice(i * TILE, (i + 1) * TILE)
        value = BETA * momentum[here].astype(jnp.float32) + summed[here].astype(jnp.float32)
        back = inverse_tile(decoded[i * rows : (i + 1) * rows], offsets[i * per : (i + 1) * per], table, back_table[...])
        out[here] = (value - back).astype(jnp.bfloat16)


def update_kernel(parts, offsets, high, low, back_table, out):
    table = (high[...], low[...])
    per = TILE // BLOCK
    rows = TILE // STRIDE
    count = parts.shape[0]
    for i in range(out.shape[0] // TILE):
        here = slice(i * rows, (i + 1) * rows)
        total = parts[0, here].astype(jnp.float32)
        for k in range(1, count):
            total += parts[k, here].astype(jnp.float32)
        back = inverse_tile(total * (1.0 / count), offsets[i * per : (i + 1) * per], table, back_table[...])
        out[i * TILE : (i + 1) * TILE] = back.astype(jnp.bfloat16)


def call(kernel, out_shape, flops, scratch=(), in_specs=None, grant=GRANT):
    extra = {} if in_specs is None else {"in_specs": in_specs}
    return pl.pallas_call(
        kernel,
        out_shape=out_shape,
        scratch_shapes=scratch,
        compiler_params=pltpu.CompilerParams(vmem_limit_bytes=grant),
        cost_estimate=pl.CostEstimate(flops=flops, bytes_accessed=2 << 20, transcendentals=0),
        **extra,
    )


def shaped(*shape, dtype=jnp.bfloat16):
    return jax.ShapeDtypeStruct(shape, dtype)


def step(features, out_grads, doc_ids, offsets, momentum):
    shards = lax.axis_size("shard")
    deep = shards // LINES
    groups = lax.axis_size("rep")

    def along_line(x, k):
        pairs = [(y * deep + z, y * deep + (z + k) % deep) for y in range(LINES) for z in range(deep)]
        return lax.ppermute(x, "shard", pairs)

    def across(x, k):
        pairs = [(y * deep + z, (y + k) % LINES * deep + z) for y in range(LINES) for z in range(deep)]
        return lax.ppermute(x, "shard", pairs)

    def exchange(x):
        lines = [[y * deep + z for z in range(deep)] for y in range(LINES)]
        return lax.all_to_all(x, "shard", 0, 0, axis_index_groups=lines, tiled=True)

    rows = features[0, 0]
    grads = out_grads[0, 0]
    tokens, panel = grads.shape
    width = rows.shape[1] // shards
    whole = pl.BlockSpec(memory_space=pltpu.VMEM)
    apart = pl.BlockSpec(memory_space=pltpu.HBM)
    work = 2 * panel * deep * tokens * width

    early = call(
        early_kernel,
        shaped(deep, tokens, panel + width),
        work,
        (pltpu.SemaphoreType.DMA((deep,)), pltpu.SemaphoreType.DMA((deep,))),
        [apart, apart],
        FULL,
    )(rows, grads)
    early = exchange(early)

    documents = lax.broadcasted_iota(jnp.int32, (DOCS, tokens), 0)
    onehot = (doc_ids[0] == documents).astype(jnp.float32)
    counts = jnp.broadcast_to(jnp.sum(onehot, axis=1, keepdims=True), (DOCS, tokens))
    before = across(counts, 1)
    after = across(counts, -1)
    lane = lax.broadcasted_iota(jnp.int32, (DOCS, tokens), 1)
    heads = jnp.where(lane == 0, counts, jnp.where(lane == 1, before, jnp.where(lane == 2, after, 0.0)))
    extra = jnp.concatenate([onehot, heads], axis=0).astype(jnp.bfloat16)

    notes = [extra]
    for k in (2, 1, 3):
        notes.append(along_line(extra, k))
    notes = [notes[0], notes[2], notes[1], notes[3]]

    third, second, first = call(
        late_kernel,
        [shaped(deep, tokens, 2 * width)] * 2 + [shaped(deep, tokens, 3 * width)],
        work,
        (pltpu.SemaphoreType.DMA((7 * deep,)),),
        [apart],
        FULL,
    )(rows)
    third = exchange(third)
    second = exchange(second)
    first = exchange(first)

    weights = call(scale_kernel, shaped(panel, deep * tokens), work)(early, *notes)
    half = panel // 2
    up, down = call(far_kernel, [shaped(half, width)] * 2, work)(weights, early)

    def ring(up, down):
        up = across(up, 1)
        down = across(down, -1)
        return up, down

    def near(start, top, received, exchanged):
        kernel = functools.partial(near_kernel, start, top)
        return call(kernel, shaped(panel, width), work)(weights, received, exchanged)

    def both(up, down, exchanged):
        return near(0, True, up, exchanged), near(width, False, down, exchanged)

    up, down = ring(up, down)
    up, down = ring(*both(up, down, third))
    up, down = ring(*both(up, down, second))
    up = near(0, True, up, first)
    down = near(width, False, down, first)
    up, down = ring(up, down)

    high, low, ahead, back = dct_parts()
    ones = jnp.asarray(np.kron(np.eye(TILE // BLOCK), np.ones((BLOCK, BLOCK))), jnp.bfloat16)
    wide = jnp.repeat(offsets[0], BLOCK, axis=1)
    kept = panel // STRIDE
    flops = 6 * 2 * 2 * panel * TILE * TILE
    tables = (high, low, ahead, ones)
    product = call(own_kernel, shaped(panel, width, dtype=jnp.float32), work)(weights, first)
    near_by = (momentum[0], wide, *tables)
    momentum_near, wide_near, *tables_near = call(
        keep_kernel, [shaped(*x.shape, dtype=x.dtype) for x in near_by], work // 8
    )(*near_by)
    summed, decoded, sent = pl.pallas_call(
        forward_kernel,
        out_shape=(shaped(panel, width), shaped(kept, width, dtype=jnp.float32), shaped(groups, kept, width)),
        in_specs=[whole, apart, apart] + [whole] * 6,
        out_specs=(apart, whole, whole),
        scratch_shapes=(
            pltpu.VMEM((kept, width), jnp.float32),
            pltpu.VMEM((panel, width), jnp.bfloat16),
            pltpu.VMEM((2, panel, width), jnp.bfloat16),
            pltpu.SemaphoreType.DMA((3, panel // TILE)),
        ),
        compiler_params=pltpu.CompilerParams(vmem_limit_bytes=GRANT),
        cost_estimate=pl.CostEstimate(flops=flops, bytes_accessed=2 << 20, transcendentals=0),
    )(product, up, down, momentum_near, wide_near, *tables_near)
    parts = lax.all_to_all(sent, "rep", 0, 0, tiled=True)
    residual = call(residual_kernel, shaped(panel, width), flops)(momentum[0], summed, decoded, wide, high, low, back)
    update = call(update_kernel, shaped(panel, width), flops)(parts, wide, high, low, back)
    return residual[None], update[None]


def solution(mesh):
    return jax.shard_map(
        step,
        mesh=mesh,
        in_specs=(
            P(None, "rep", "shard", None),
            P(None, "rep", "shard", None),
            P(None, "rep", "shard"),
            P(None, None, "shard"),
            P("rep", None, "shard"),
        ),
        out_specs=(P("rep", None, "shard"), P(None, None, "shard")),
        check_vma=False,
    )
```

```python
import functools
import math

import jax
import jax.numpy as jnp
import numpy as np
from jax import lax
from jax.experimental import pallas as pl
from jax.experimental.pallas import tpu as pltpu
from jax.sharding import PartitionSpec as P


BLOCK = 64
STRIDE = 16
DOCS = 16
LINES = 8
BETA = 0.9
CLIP = 2.0
EPS = 1e-06


TILE = 256
GRANT = 16 << 20
FULL = 60 << 20


def dct_parts():
    freq = np.arange(BLOCK, dtype=np.float64)[:, None]
    place = np.arange(BLOCK, dtype=np.float64)[None, :]
    table = np.cos(math.pi * (2.0 * place + 1.0) * freq / (2.0 * BLOCK)) * math.sqrt(2.0 / BLOCK)
    table[0] /= math.sqrt(2.0)
    whole = np.kron(np.eye(TILE // BLOCK), table)
    high = whole.astype(jnp.bfloat16)
    low = (whole - high.astype(np.float64)).astype(jnp.bfloat16)
    some = slice(0, BLOCK)
    ahead = np.concatenate([high[some, some], high[some, some], low[some, some]], axis=1)
    back = np.concatenate([high[some, some].T, high[some, some].T, low[some, some].T], axis=1)
    return tuple(jnp.asarray(part) for part in (high, low, ahead, back))


def dot(a, b, dims):
    return lax.dot_general(a, b, (dims, ((), ())), preferred_element_type=jnp.float32)


def split(x):
    high = x.astype(jnp.bfloat16)
    return high, (x - high.astype(jnp.float32)).astype(jnp.bfloat16)


def left(table, x):
    high, low = split(x)
    dims = ((1,), (0,))
    out = []
    for i in range(x.shape[0] // BLOCK):
        here = slice(i * BLOCK, (i + 1) * BLOCK)
        out.append(dot(table, jnp.concatenate([high[here], low[here], high[here]], axis=0), dims))
    return jnp.concatenate(out, axis=0)


def right(x, table, dim):
    (th, tl), (xh, xl) = table, split(x)
    dims = ((1,), (dim,))
    return dot(xh, th, dims) + (dot(xl, th, dims) + dot(xh, tl, dims))


def selected(offsets):
    count, width = offsets.shape
    shape = (count, BLOCK, width)
    both = lax.broadcasted_iota(jnp.int32, shape, 1) + lax.broadcasted_iota(jnp.int32, shape, 2)
    return ((both & (STRIDE - 1)) == offsets[:, None, :]).reshape(count * BLOCK, width)


def gathered(exchanged, start, size):
    deep = exchanged.shape[0]
    z = lax.axis_index("shard") % deep
    return jnp.concatenate([exchanged[(z - k + deep) % deep, :, start : start + size] for k in range(deep)], axis=0)


def fetch(rows, deep, width, moves, sem):
    me = lax.axis_index("shard")
    line = me // deep
    copies = []
    for i, (owner, z, target) in enumerate(moves):
        block = (line + owner + LINES) % LINES * deep + z
        column = pl.multiple_of(block * width, width)
        copies.append(pltpu.make_async_copy(rows.at[:, pl.ds(column, width)], target, sem.at[i]))
    for copy in copies:
        copy.start()
    return copies


def early_kernel(rows, grads, out, sem, given):
    deep = out.shape[0]
    panel = grads.shape[1]
    width = out.shape[2] - panel
    moves = [(4, z, out.at[z, :, pl.ds(panel, width)]) for z in range(deep)]
    copies = fetch(rows, deep, width, moves, sem)
    for z in range(deep):
        copies.append(pltpu.make_async_copy(grads, out.at[z, :, pl.ds(0, panel)], given.at[z]))
        copies[-1].start()
    for copy in copies:
        copy.wait()


def late_kernel(rows, third, second, first, sem):
    deep = third.shape[0]
    width = third.shape[2] // 2
    moves = []
    for target, owners in ((third, (3, -3)), (second, (2, -2)), (first, (1, -1, 0))):
        for z in range(deep):
            for j, owner in enumerate(owners):
                moves.append((owner, z, target.at[z, :, pl.ds(j * width, width)]))
    for copy in fetch(rows, deep, width, moves, sem):
        copy.wait()


def scale_kernel(exchanged, *rest):
    notes, out = rest[:-1], rest[-1]
    deep, tokens = exchanged.shape[0], exchanged.shape[1]
    panel = out.shape[0]
    z = lax.axis_index("shard") % deep
    marks = [note[...].astype(jnp.float32) for note in notes]
    heads = marks[0][DOCS:]
    for mark in marks[1:]:
        heads = heads + mark[DOCS:]
    share = 1.0 / jnp.maximum(jnp.sum(heads, axis=1, keepdims=True), 1.0)
    for k in range(deep):
        weight = jnp.sum(marks[k][:DOCS] * share, axis=0, keepdims=True)
        block = exchanged[(z - k + deep) % deep, :, :panel].astype(jnp.float32)
        out[:, k * tokens : (k + 1) * tokens] = (block.T * weight).astype(jnp.bfloat16)


def far_kernel(weights, exchanged, up, down):
    half = up.shape[0]
    columns = gathered(exchanged, exchanged.shape[2] - up.shape[1], up.shape[1])
    dims = ((1,), (0,))
    up[...] = dot(weights[:half], columns, dims).astype(jnp.bfloat16)
    down[...] = dot(weights[half:], columns, dims).astype(jnp.bfloat16)


def near_kernel(start, top, weights, received, exchanged, out):
    width = out.shape[1]
    total = dot(weights[...], gathered(exchanged, start, width), ((1,), (0,)))
    rows = received.shape[0]
    if rows == out.shape[0]:
        out[...] = (total + received[...].astype(jnp.float32)).astype(jnp.bfloat16)
    else:
        here, other = (slice(0, rows), slice(rows, None)) if top else (slice(rows, None), slice(0, rows))
        out[here] = (total[here] + received[...].astype(jnp.float32)).astype(jnp.bfloat16)
        out[other] = total[other].astype(jnp.bfloat16)


def base_kernel(weights, exchanged, momentum, offsets, *rest):
    tables, (product, kept, offsets_out, *tables_out) = rest[: len(rest) // 2 - 1], rest[len(rest) // 2 - 1 :]
    product[...] = dot(weights[...], gathered(exchanged, 2 * product.shape[1], product.shape[1]), ((1,), (0,)))
    kept[...] = momentum[...]
    offsets_out[...] = offsets[...]
    for table, out in zip(tables, tables_out):
        out[...] = table[...]


def forward_kernel(
    product, up, down, momentum, offsets, high, low, ahead, ones, summed, decoded, sent, packed, held, parts, sem
):
    table = (high[...], low[...])
    per = TILE // BLOCK
    rows = TILE // STRIDE
    fetches = []
    for i in range(product.shape[0] // TILE):
        there = pl.ds(i * TILE, TILE)
        pair = [pltpu.make_async_copy(x.at[there], parts.at[j, there], sem.at[1 + j, i]) for j, x in enumerate((up, down))]
        fetches.append(pair)
        for copy in pair:
            copy.start()
    copies = []
    for i in range(product.shape[0] // TILE):
        here = slice(i * TILE, (i + 1) * TILE)
        for copy in fetches[i]:
            copy.wait()
        total = product[here] + parts[0, here].astype(jnp.float32) + parts[1, here].astype(jnp.float32)
        gradient = total.astype(jnp.bfloat16)
        held[here] = gradient
        copies.append(pltpu.make_async_copy(held.at[pl.ds(i * TILE, TILE)], summed.at[pl.ds(i * TILE, TILE)], sem.at[0, i]))
        copies[-1].start()
        value = BETA * momentum[here].astype(jnp.float32) + gradient.astype(jnp.float32)
        spectrum = right(left(ahead[...], value), table, 1)
        kept = jnp.where(selected(offsets[i * per : (i + 1) * per]), spectrum, 0.0)
        packed[i * rows : (i + 1) * rows] = jnp.sum(kept.reshape(rows, STRIDE, TILE), axis=1)
    values = packed[...]
    group = BLOCK // STRIDE
    squares = jnp.sum((values * values).reshape(-1, group, TILE), axis=1)
    first = squares.astype(jnp.bfloat16)
    rest = squares - first.astype(jnp.float32)
    second, third = split(rest)
    dims = ((1,), (0,))
    total = dot(first, ones[...], dims) + (dot(second, ones[...], dims) + dot(third, ones[...], dims))
    mean = total * (1.0 / (BLOCK * group))
    scale = (CLIP * jnp.sqrt(mean + EPS)).astype(jnp.bfloat16).astype(jnp.float32)
    spread = jnp.broadcast_to(scale[:, None, :], (scale.shape[0], group, TILE)).reshape(values.shape)
    quantized = jnp.clip(values / spread, -1.0, 1.0).astype(jnp.bfloat16)
    result = quantized.astype(jnp.float32) * spread
    decoded[...] = result
    rounded = result.astype(jnp.bfloat16)
    for k in range(sent.shape[0]):
        sent[k] = rounded
    for copy in copies:
        copy.wait()


def spread_tile(values, offsets):
    rows, width = values.shape
    wide = jnp.broadcast_to(values[:, None, :], (rows, STRIDE, width)).reshape(rows * STRIDE, width)
    return jnp.where(selected(offsets), wide, 0.0)


def inverse_tile(values, offsets, table, back):
    return right(left(back, spread_tile(values, offsets)), table, 0)


def residual_kernel(momentum, summed, decoded, offsets, high, low, back_table, out):
    table = (high[...], low[...])
    per = TILE // BLOCK
    rows = TILE // STRIDE
    for i in range(out.shape[0] // TILE):
        here = slice(i * TILE, (i + 1) * TILE)
        value = BETA * momentum[here].astype(jnp.float32) + summed[here].astype(jnp.float32)
        back = inverse_tile(decoded[i * rows : (i + 1) * rows], offsets[i * per : (i + 1) * per], table, back_table[...])
        out[here] = (value - back).astype(jnp.bfloat16)


def update_kernel(parts, offsets, high, low, back_table, out):
    table = (high[...], low[...])
    per = TILE // BLOCK
    rows = TILE // STRIDE
    count = parts.shape[0]
    for i in range(out.shape[0] // TILE):
        here = slice(i * rows, (i + 1) * rows)
        total = parts[0, here].astype(jnp.float32)
        for k in range(1, count):
            total += parts[k, here].astype(jnp.float32)
        back = inverse_tile(total * (1.0 / count), offsets[i * per : (i + 1) * per], table, back_table[...])
        out[i * TILE : (i + 1) * TILE] = back.astype(jnp.bfloat16)


def call(kernel, out_shape, flops, scratch=(), in_specs=None, grant=GRANT):
    extra = {} if in_specs is None else {"in_specs": in_specs}
    return pl.pallas_call(
        kernel,
        out_shape=out_shape,
        scratch_shapes=scratch,
        compiler_params=pltpu.CompilerParams(vmem_limit_bytes=grant),
        cost_estimate=pl.CostEstimate(flops=flops, bytes_accessed=2 << 20, transcendentals=0),
        **extra,
    )


def shaped(*shape, dtype=jnp.bfloat16):
    return jax.ShapeDtypeStruct(shape, dtype)


def step(features, out_grads, doc_ids, offsets, momentum):
    shards = lax.axis_size("shard")
    deep = shards // LINES
    groups = lax.axis_size("rep")

    def along_line(x, k):
        pairs = [(y * deep + z, y * deep + (z + k) % deep) for y in range(LINES) for z in range(deep)]
        return lax.ppermute(x, "shard", pairs)

    def across(x, k):
        pairs = [(y * deep + z, (y + k) % LINES * deep + z) for y in range(LINES) for z in range(deep)]
        return lax.ppermute(x, "shard", pairs)

    def exchange(x):
        lines = [[y * deep + z for z in range(deep)] for y in range(LINES)]
        return lax.all_to_all(x, "shard", 0, 0, axis_index_groups=lines, tiled=True)

    rows = features[0, 0]
    grads = out_grads[0, 0]
    tokens, panel = grads.shape
    width = rows.shape[1] // shards
    whole = pl.BlockSpec(memory_space=pltpu.VMEM)
    apart = pl.BlockSpec(memory_space=pltpu.HBM)
    work = 2 * panel * deep * tokens * width

    early = call(
        early_kernel,
        shaped(deep, tokens, panel + width),
        work,
        (pltpu.SemaphoreType.DMA((deep,)), pltpu.SemaphoreType.DMA((deep,))),
        [apart, apart],
        FULL,
    )(rows, grads)
    early = exchange(early)

    documents = lax.broadcasted_iota(jnp.int32, (DOCS, tokens), 0)
    onehot = (doc_ids[0] == documents).astype(jnp.float32)
    counts = jnp.broadcast_to(jnp.sum(onehot, axis=1, keepdims=True), (DOCS, tokens))
    before = across(counts, 1)
    after = across(counts, -1)
    lane = lax.broadcasted_iota(jnp.int32, (DOCS, tokens), 1)
    heads = jnp.where(lane == 0, counts, jnp.where(lane == 1, before, jnp.where(lane == 2, after, 0.0)))
    extra = jnp.concatenate([onehot, heads], axis=0).astype(jnp.bfloat16)

    notes = [extra]
    for k in (2, 1, 3):
        notes.append(along_line(extra, k))
    notes = [notes[0], notes[2], notes[1], notes[3]]

    third, second, first = call(
        late_kernel,
        [shaped(deep, tokens, 2 * width)] * 2 + [shaped(deep, tokens, 3 * width)],
        work,
        (pltpu.SemaphoreType.DMA((7 * deep,)),),
        [apart],
        FULL,
    )(rows)
    third = exchange(third)
    second = exchange(second)
    first = exchange(first)

    weights = call(scale_kernel, shaped(panel, deep * tokens), work)(early, *notes)
    half = panel // 2
    up, down = call(far_kernel, [shaped(half, width)] * 2, work)(weights, early)

    def ring(up, down):
        up = across(up, 1)
        down = across(down, -1)
        return up, down

    def near(start, top, received, exchanged):
        kernel = functools.partial(near_kernel, start, top)
        return call(kernel, shaped(panel, width), work)(weights, received, exchanged)

    def both(up, down, exchanged):
        return near(0, True, up, exchanged), near(width, False, down, exchanged)

    up, down = ring(up, down)
    up, down = ring(*both(up, down, third))
    up, down = ring(*both(up, down, second))
    up, down = ring(*both(up, down, first))

    high, low, ahead, back = dct_parts()
    ones = jnp.asarray(np.kron(np.eye(TILE // BLOCK), np.ones((BLOCK, BLOCK))), jnp.bfloat16)
    wide = jnp.repeat(offsets[0], BLOCK, axis=1)
    kept = panel // STRIDE
    flops = 6 * 2 * 2 * panel * TILE * TILE
    tables = (high, low, ahead, ones)
    product, momentum_near, wide_near, *tables_near = call(
        base_kernel,
        [shaped(panel, width, dtype=jnp.float32), shaped(panel, width), shaped(*wide.shape, dtype=jnp.int32)]
        + [shaped(*table.shape) for table in tables],
        work,
    )(weights, first, momentum[0], wide, *tables)
    summed, decoded, sent = pl.pallas_call(
        forward_kernel,
        out_shape=(shaped(panel, width), shaped(kept, width, dtype=jnp.float32), shaped(groups, kept, width)),
        in_specs=[whole, apart, apart] + [whole] * 6,
        out_specs=(apart, whole, whole),
        scratch_shapes=(
            pltpu.VMEM((kept, width), jnp.float32),
            pltpu.VMEM((panel, width), jnp.bfloat16),
            pltpu.VMEM((2, panel, width), jnp.bfloat16),
            pltpu.SemaphoreType.DMA((3, panel // TILE)),
        ),
        compiler_params=pltpu.CompilerParams(vmem_limit_bytes=GRANT),
        cost_estimate=pl.CostEstimate(flops=flops, bytes_accessed=2 << 20, transcendentals=0),
    )(product, up, down, momentum_near, wide_near, *tables_near)
    parts = lax.all_to_all(sent, "rep", 0, 0, tiled=True)
    residual = call(residual_kernel, shaped(panel, width), flops)(momentum[0], summed, decoded, wide, high, low, back)
    update = call(update_kernel, shaped(panel, width), flops)(parts, wide, high, low, back)
    return residual[None], update[None]


def solution(mesh):
    return jax.shard_map(
        step,
        mesh=mesh,
        in_specs=(
            P(None, "rep", "shard", None),
            P(None, "rep", "shard", None),
            P(None, "rep", "shard"),
            P(None, None, "shard"),
            P("rep", None, "shard"),
        ),
        out_specs=(P("rep", None, "shard"), P(None, None, "shard")),
        check_vma=False,
    )
```
